256 devices in a mesh: row: 8 (over z_lo, y), col: 32 (over z_hi, x, core).
Axes of the slice: x: 4, y: 4, z: 8 (z_hi: 4, z_lo: 2; z = z_hi * 2 + z_lo), core: 2. Of those that a mesh axis runs over, the one named last changes fastest.
Arguments:
- alignment: float32 [512, 768, 256], P('row', 'col'), may hold values from -40 to 40
- seq_mask: int32 [512], replicated, may hold values 0 or 1
- res_mask: int32 [768], replicated, may hold values 0 or 1
- attn_gain: float32 [256], replicated, may hold values from 0.5 to 1.5
- outer_product_gain: float32 [256], replicated, may hold values from 0.5 to 1.5
- w_query: bfloat16 [256, 256], replicated, may hold values from -24 to 24
- w_key: bfloat16 [256, 256], replicated, may hold values from -2 to 2
- w_value: bfloat16 [256, 256], replicated, may hold values from -0.375 to 0.375
- w_gate: bfloat16 [256, 256], replicated, may hold values from -0.375 to 0.375
- output_weight: bfloat16 [256, 256], replicated, may hold values from -0.375 to 0.375
- w_left: bfloat16 [256, 32], replicated, may hold values from -0.375 to 0.375
- w_right: bfloat16 [256, 32], replicated, may hold values from -0.375 to 0.375
- w_pair: bfloat16 [1024, 128], replicated, may hold values from -3 to 3
Outputs:
- alignment_output: float32 [512, 768, 256], P('row', 'col')
- pair_increment: float32 [768, 768, 128], P('row', 'col')
The draws below stay inside these ranges and needn't reach their ends.
All inputs are finite; a program needn't handle non-finite values.
Results may differ from the reference program's by a relative error of at most 0.0095.
Values may be sent and summed in bfloat16 or wider, within the bound.
No kernel may reach another device: no remote copies, remote signals or barrier semaphores. Data moves between devices by JAX's collectives and lax.ppermute only.
A program may use at most 128 MiB of HBM per device.

```python
import math
import jax
import jax.numpy as jnp
from jax import lax

C = 256
HEADS = 8
HEAD_DIM = 32
COPM = 32
CZ = 128
SEQS = 512
RES = 768


def draw_alignment(key, part):
    normals = jax.random.normal(jax.random.fold_in(key, 1), (SEQS, RES, C), jnp.float32)
    return jnp.clip(normals, -6.0, 6.0)


def key_matrix(key):
    entries = jax.random.normal(jax.random.fold_in(key, 7), (C, HEADS * HEAD_DIM), jnp.float32) / math.sqrt(C)
    return jnp.clip(entries, -6.0 / math.sqrt(C), 6.0 / math.sqrt(C))


def draw_w_key(key, part):
    return key_matrix(key).astype(jnp.bfloat16)


def draw_w_query(key, part):
    independent = key_matrix(jax.random.fold_in(key, 3))
    return independent.astype(jnp.bfloat16)


def touch_ends(array, rng, least, largest):
    place = [jax.random.randint(jax.random.fold_in(rng, axis), (), 0, length) for axis, length in enumerate(array.shape)]
    widest = array.shape.index(max(array.shape))
    neighbour = place[:widest] + [(place[widest] + 1) % array.shape[widest]] + place[widest + 1:]
    return array.at[tuple(place)].set(least).at[tuple(neighbour)].set(largest)


def scatter_about(key, dims, width, limit, kind=jnp.bfloat16):
    values = width * jax.random.normal(key, dims, jnp.float32)
    return jnp.clip(values, min=-limit, max=limit).astype(kind)


def setup_inputs(seed: int = 0) -> dict:
    streams_of = jax.random.split(jax.random.key(seed), 14)
    alignment = draw_alignment(jax.random.fold_in(streams_of[13], 71), 0)
    seq_mask = touch_ends((jax.random.randint(streams_of[1], (SEQS,), 0, 8) < 7).astype(jnp.int32), jax.random.fold_in(streams_of[1], 1), 0, 1)
    res_mask = touch_ends((jax.random.randint(streams_of[2], (RES,), 0, 8) < 7).astype(jnp.int32), jax.random.fold_in(streams_of[2], 1), 0, 1)
    attn_gain = jnp.clip(1.0 + 0.1 * jax.random.normal(streams_of[3], (C,), jnp.float32), 0.5, 1.5)
    outer_product_gain = jnp.clip(1.0 + 0.1 * jax.random.normal(streams_of[4], (C,), jnp.float32), 0.5, 1.5)
    w_query = draw_w_query(jax.random.fold_in(streams_of[13], 71), 0)
    w_key = draw_w_key(jax.random.fold_in(streams_of[13], 71), 0)
    w_value = scatter_about(streams_of[7], (C, HEADS * HEAD_DIM), C ** -0.5, 0.375)
    w_gate = scatter_about(streams_of[8], (C, HEADS * HEAD_DIM), C ** -0.5, 0.375)
    output_weight = scatter_about(streams_of[9], (HEADS * HEAD_DIM, C), (HEADS * HEAD_DIM) ** -0.5, 0.375)
    w_left = scatter_about(streams_of[10], (C, COPM), C ** -0.5, 0.375)
    w_right = scatter_about(streams_of[11], (C, COPM), C ** -0.5, 0.375)
    w_pair = scatter_about(streams_of[12], (COPM * COPM, CZ), 0.5, 3.0)
    return dict(alignment=alignment, seq_mask=seq_mask, res_mask=res_mask, attn_gain=attn_gain, outer_product_gain=outer_product_gain, w_query=w_query, w_key=w_key, w_value=w_value, w_gate=w_gate, output_weight=output_weight, w_left=w_left, w_right=w_right, w_pair=w_pair)


def normalized_rows(values, gains):
    average = lax.optimization_barrier(jnp.mean(values, -1, keepdims=True))
    centred = values - average
    spread = lax.optimization_barrier(jnp.mean(centred * centred, -1, keepdims=True))
    return centred * lax.rsqrt(spread + 1e-05) * gains

def reference(alignment, seq_mask, res_mask, attn_gain, outer_product_gain, w_query, w_key, w_value, w_gate, output_weight, w_left, w_right, w_pair):
    sequence_total, residue_total, channel_width = alignment.shape
    hidden = w_query.shape[1]
    normed = normalized_rows(alignment, attn_gain).astype(jnp.bfloat16).reshape(-1, channel_width)
    query_scale = HEAD_DIM ** (-0.5)
    queries = (jnp.dot(normed, w_query, preferred_element_type=jnp.float32) * query_scale).astype(jnp.bfloat16)
    key_rows = jnp.dot(normed, w_key, preferred_element_type=jnp.float32).astype(jnp.bfloat16)
    value_rows = jnp.dot(normed, w_value, preferred_element_type=jnp.float32).astype(jnp.bfloat16)
    gate_lin = jnp.dot(normed, w_gate, preferred_element_type=jnp.float32)
    key_bias = jnp.where(seq_mask > 0, 0.0, -1000000000.0).astype(jnp.float32)

    def arrange(values):
        return values.reshape(sequence_total, residue_total, -1).transpose(1, 0, 2)

    def column(column_parts):
        col_query, col_key, col_value, col_gate = column_parts
        heads_query = col_query.reshape(sequence_total, HEADS, HEAD_DIM).astype(jnp.float32)
        heads_key = col_key.reshape(sequence_total, HEADS, HEAD_DIM).astype(jnp.float32)
        heads_value = col_value.reshape(sequence_total, HEADS, HEAD_DIM).astype(jnp.float32)
        logits = jnp.einsum('shd,thd->hst', heads_query, heads_key) + key_bias[None, None, :]
        weights = jax.nn.softmax(logits, axis=-1).astype(jnp.bfloat16)
        attended = jnp.einsum('hst,thd->shd', weights.astype(jnp.float32), heads_value).reshape(sequence_total, hidden)
        return (jax.nn.sigmoid(col_gate) * attended).astype(jnp.bfloat16)
    gated_output = lax.map(column, (arrange(queries), arrange(key_rows), arrange(value_rows), arrange(gate_lin)))
    gated_output = gated_output.transpose(1, 0, 2).reshape(-1, hidden)
    alignment_output = alignment + jnp.dot(gated_output, output_weight, preferred_element_type=jnp.float32).reshape(sequence_total, residue_total, channel_width)
    second_normalized = normalized_rows(alignment_output, outer_product_gain).astype(jnp.bfloat16).reshape(-1, channel_width)
    side_mask = (seq_mask[:, None] * res_mask[None, :]).astype(jnp.float32)[:, :, None]
    left = (jnp.dot(second_normalized, w_left, preferred_element_type=jnp.float32).reshape(sequence_total, residue_total, COPM) * side_mask).astype(jnp.bfloat16).reshape(sequence_total, -1)
    right = (jnp.dot(second_normalized, w_right, preferred_element_type=jnp.float32).reshape(sequence_total, residue_total, COPM) * side_mask).astype(jnp.bfloat16).reshape(sequence_total, -1)
    live_total = jnp.sum(seq_mask)
    block_rows = 32
    contraction = (((0,), (0,)), ((), ()))

    def pair_block(offset):
        left_part = lax.dynamic_slice_in_dim(left, (offset * COPM).astype(jnp.int32), block_rows * COPM, 1)
        products = lax.dot_general(left_part, right, contraction, preferred_element_type=jnp.float32)
        outer_sum = products.reshape(block_rows, COPM, residue_total, COPM).transpose(0, 2, 1, 3).reshape(-1, COPM * COPM).astype(jnp.bfloat16)
        projected_output = jnp.dot(outer_sum, w_pair, preferred_element_type=jnp.float32).reshape(block_rows, residue_total, -1)
        block_mask = lax.dynamic_slice_in_dim(res_mask, offset.astype(jnp.int32), block_rows, 0)
        count_values = jnp.maximum(live_total * block_mask[:, None] * res_mask[None, :], 1).astype(jnp.float32)
        return projected_output / count_values[:, :, None]
    offsets = jnp.arange(residue_total // block_rows, dtype=jnp.int32) * block_rows
    pair_increment = lax.map(pair_block, offsets).reshape(residue_total, residue_total, -1)
    return (alignment_output, pair_increment)
```

```python
import jax
import jax.numpy as jnp
import numpy as np
from jax import lax
from jax.experimental import pallas as pl
from jax.experimental.pallas import tpu as pltpu
from jax.sharding import PartitionSpec as P

HEADS = 8
HEAD_DIM = 32
ROWS = 8
COLS = 32
SEQ = 64
RES = 24
OWN = RES // ROWS
TOTAL = SEQ * ROWS
PAIR_ROWS = RES * COLS // ROWS
BLOCK = OWN * SEQ
GROUP = 4
SIDE = OWN * 32
C = 256
COPM = 32
CZ = 128
EPS = 1e-05
BF = jnp.bfloat16
F32 = jnp.float32
VMEM = pl.BlockSpec(memory_space=pltpu.VMEM)
SMEM = pl.BlockSpec(memory_space=pltpu.SMEM)


def dot(a, b):
    return jnp.dot(a, b, preferred_element_type=F32)


def iota(shape, dim):
    return lax.broadcasted_iota(jnp.int32, shape, dim)


def norm_kernel(rank_ref, align_ref, gain_ref, *refs):
    outs, halves = refs[:ROWS], refs[ROWS:]
    for i in range(2):
        halves[i][...] = align_ref[:, i * 128 : (i + 1) * 128]
    rank = rank_ref[0]
    gain = gain_ref[...]
    row = iota((SEQ, 128), 0)
    lane = iota((SEQ, 128), 1)
    row16 = iota((16, 128), 0)
    for n in range(ROWS):
        first = lax.rem(rank + n, ROWS) * OWN
        extra = jnp.zeros((16, 128), F32)
        for j in range(OWN):
            x = jnp.concatenate([half[pl.ds(first + j, SEQ, stride=RES), :] for half in halves], 1)
            centred = x - jnp.mean(x, -1, keepdims=True)
            spread = jnp.mean(centred * centred, -1, keepdims=True) + EPS
            normed = centred * lax.rsqrt(spread) * gain
            outs[n][j * SEQ : (j + 1) * SEQ, :] = normed.astype(BF)
            sigma = jnp.sqrt(spread)
            high = sigma.astype(BF).astype(F32)
            low = sigma - high
            spots = jnp.where(lane == row, high, jnp.where(lane == row + SEQ, low, 0.0))
            extra = extra + jnp.where(row16 == j, jnp.sum(spots, 0, keepdims=True), 0.0)
        outs[n][BLOCK : BLOCK + 16, 0:128] = extra.astype(BF)
        outs[n][BLOCK : BLOCK + 16, 128:256] = jnp.zeros((16, 128), BF)


def attend_kernel(*refs):
    rank_ref, live_ref = refs[:2]
    blocks = refs[2:10]
    (wq_ref, wk_ref, wv_ref, wg_ref, wo_ref, inv_gain_ref, gain2_ref, wlr_ref, bias_ref, mask_ref) = refs[10:20]
    gated_outs = refs[20:28]
    left_ref, right_ref = refs[28:30]
    gated_ref = refs[30]
    gate_ref = refs[31]
    rank = rank_ref[0]
    lane_head = iota((1, C), 1) // HEAD_DIM
    half = iota((1, 128), 1) < SEQ
    for j in range(OWN):
        x = jnp.concatenate([b[j * SEQ : (j + 1) * SEQ, :] for b in blocks], 0)
        xt = x.T
        keys = dot(x, wk_ref[...]).astype(BF)
        qt = (dot(wq_ref[...], xt) * HEAD_DIM**-0.5).astype(BF)
        vt = dot(wv_ref[...], xt).astype(BF)
        gate_ref[...] = jax.nn.sigmoid(dot(wg_ref[...], xt))
        for h in range(HEADS):
            own = slice(h * HEAD_DIM, (h + 1) * HEAD_DIM)
            head_keys = keys * (lane_head == h).astype(BF)
            for s in range(TOTAL // C):
                cols = slice(s * C, (s + 1) * C)
                logits = dot(head_keys, qt[:, cols]) + bias_ref[...]
                top = jnp.max(logits, 0, keepdims=True)
                weights = jnp.exp(logits - top)
                total = jnp.sum(weights, 0, keepdims=True)
                mixed = dot(vt[own, :], weights.astype(BF)) / total
                gated_ref[own, cols] = (mixed * gate_ref[own, cols]).astype(BF)
        gated = gated_ref[...]
        rows = gated.T
        for p in range(ROWS):
            gated_outs[p][j * SEQ : (j + 1) * SEQ, :] = rows[p * SEQ : (p + 1) * SEQ, :]
        pieces = []
        for p in range(0, ROWS, 2):
            tiles = []
            for b in blocks[p : p + 2]:
                tile = b[BLOCK : BLOCK + 16, 0:128].astype(F32)[j : j + 1]
                tiles.append(tile + pltpu.roll(tile, SEQ, 1))
            pieces.append(jnp.where(half, tiles[0], tiles[1]))
        sigma = jnp.concatenate(pieces, 1)
        y = dot(wo_ref[...], gated) + xt.astype(F32) * inv_gain_ref[...] * sigma
        centred = y - jnp.mean(y, 0, keepdims=True)
        spread = jnp.mean(centred * centred, 0, keepdims=True)
        second = (centred * lax.rsqrt(spread + EPS) * gain2_ref[...]).astype(BF)
        live = live_ref[j].astype(F32)
        sides = dot(wlr_ref[...], second) * (mask_ref[...] * live)
        sides = pltpu.roll(sides, rank * SEQ, 1).astype(BF)
        left_ref[j * COPM : (j + 1) * COPM, :] = sides[:COPM]
        right_ref[j * COPM : (j + 1) * COPM, :] = sides[COPM:]


def add_kernel(rank_ref, align_ref, wo_ref, *refs):
    out_ref, halves = refs[-3], refs[-2:]
    rank = rank_ref[0]
    for n in range(ROWS):
        first = lax.rem(rank + ROWS - n, ROWS) * OWN
        delta = dot(refs[n][...], wo_ref[...])
        for j in range(OWN):
            for i in range(2):
                part = delta[j * SEQ : (j + 1) * SEQ, i * 128 : (i + 1) * 128]
                halves[i][pl.ds(first + j, SEQ, stride=RES), :] = part
    for i in range(2):
        lanes = slice(i * 128, (i + 1) * 128)
        out_ref[:, lanes] = align_ref[:, lanes] + halves[i][...]


def widen_kernel(w_ref, out_ref, wide_ref):
    wide_ref[...] = w_ref[...].astype(F32)
    out_ref[...] = jnp.zeros(out_ref.shape, BF)
    for b in range(COPM):
        part = wide_ref[pl.ds(b, COPM, stride=COPM), :].astype(BF)
        for i in range(GROUP):
            start = b * GROUP * COPM + i * COPM
            out_ref[start : start + COPM, i * CZ : (i + 1) * CZ] = part


def pair_kernel(scalars_ref, rows_live_ref, order_ref, inverse_ref, wide_ref, *refs):
    rights = refs[:ROWS]
    lefts = refs[ROWS:-5]
    out_ref, left_ref, stack_ref, right_ref, mid_ref = refs[-5:]
    rank = scalars_ref[0]
    for n in range(ROWS):
        start = pl.multiple_of(lax.rem(rank + ROWS - n, ROWS) * SIDE, 16)
        stack_ref[pl.ds(start, SIDE), :] = rights[n][...]
    pick = (order_ref[...] == iota((RES * COPM, RES * COPM), 1)).astype(BF)
    right_ref[...] = dot(pick, stack_ref[...]).astype(BF)
    spot = 0
    for left in lefts:
        for m in range(left.shape[0] // SIDE):
            start = pl.multiple_of(scalars_ref[1 + spot] * SIDE, 16)
            left_ref[pl.ds(start, SIDE), :] = left[m * SIDE : (m + 1) * SIDE, :]
            spot += 1
    for t in range(PAIR_ROWS * COPM // C):
        block = lax.dot_general(
            right_ref[...], left_ref[t * C : (t + 1) * C, :], (((1,), (1,)), ((), ())), preferred_element_type=F32
        )
        for b in range(COPM):
            rows = block[b * RES : (b + 1) * RES]
            mid_ref[t * 2 * RES : (t + 1) * 2 * RES, b * 128 : (b + 1) * 128] = jnp.concatenate(
                [rows[:, :128], rows[:, 128:]], 0
            ).astype(BF)
    inverse = inverse_ref[...]
    for half in range(2):
        block = dot(mid_ref[...], wide_ref[:, half * C : (half + 1) * C])
        for t in range(PAIR_ROWS // GROUP):
            for i in range(2):
                res = t * GROUP + half * 2 + i
                scale = jnp.where(rows_live_ref[res] > 0, inverse, 1.0)
                out_ref[res] = block[t * RES : (t + 1) * RES, i * CZ : (i + 1) * CZ] * scale


def shift(axis_size, n):
    return [(d, (d + n) % axis_size) for d in range(axis_size)]


def shift_z(n):
    return [(c, (c + 8 * n) % COLS) for c in range(COLS)]


def shift_x(n):
    return [(c, c // 8 * 8 + (c + 2 * n) % 8) for c in range(COLS)]


SWAP = [(c, c ^ 1) for c in range(COLS)]
SCATTER = [
    (r * COLS + c, c * ROWS // COLS * COLS + c % (COLS // ROWS) * ROWS + r) for r in range(ROWS) for c in range(COLS)
]
ORDER = np.array(
    [[j // OWN * SIDE + j % OWN * COPM + b] for b in range(COPM) for j in range(RES)], np.int32
)


def shards(
    alignment,
    seq_mask,
    res_mask,
    attn_gain,
    outer_product_gain,
    w_query,
    w_key,
    w_value,
    w_gate,
    output_weight,
    w_left,
    w_right,
    w_pair,
):
    row = lax.axis_index("row")
    col = lax.axis_index("col")
    rank = row[None].astype(jnp.int32)
    tokens = alignment.reshape(SEQ * RES, C)
    sent = pl.pallas_call(
        norm_kernel,
        out_shape=[jax.ShapeDtypeStruct((BLOCK + 16, C), BF)] * ROWS,
        in_specs=[SMEM, VMEM, VMEM],
        out_specs=[VMEM] * ROWS,
        scratch_shapes=[pltpu.VMEM((SEQ * RES, 128), F32)] * 2,
        name="norm",
    )(rank, tokens, attn_gain[None])
    blocks = [sent[0]] + [None] * (ROWS - 1)
    for n in range(1, ROWS):
        blocks[ROWS - n] = lax.ppermute(sent[n], "row", shift(ROWS, n))

    wide = pl.pallas_call(
        widen_kernel,
        out_shape=jax.ShapeDtypeStruct((COPM * GROUP * COPM, GROUP * CZ), BF),
        in_specs=[VMEM],
        out_specs=VMEM,
        scratch_shapes=[pltpu.VMEM((COPM * COPM, CZ), F32)],
        name="widen",
    )(w_pair)
    own_res = lax.dynamic_slice_in_dim(res_mask, col * RES, RES, 0)
    live = lax.dynamic_slice_in_dim(own_res, row * OWN, OWN, 0)
    seen = lax.dynamic_slice_in_dim(jnp.concatenate([seq_mask, seq_mask]), row * SEQ, TOTAL, 0)
    bias = jnp.where(seen > 0, 0.0, -1000000000.0).astype(F32)[:, None]
    mask = seen.astype(F32)[None]
    made = pl.pallas_call(
        attend_kernel,
        out_shape=[jax.ShapeDtypeStruct((BLOCK, C), BF)] * ROWS + [jax.ShapeDtypeStruct((SIDE, TOTAL), BF)] * 2,
        in_specs=[SMEM] * 2 + [VMEM] * 18,
        out_specs=[VMEM] * (ROWS + 2),
        scratch_shapes=[pltpu.VMEM((C, TOTAL), BF), pltpu.VMEM((C, TOTAL), F32)],
        name="attend",
    )(
        rank,
        live,
        *blocks,
        w_query.T,
        w_key,
        w_value.T,
        w_gate.T,
        output_weight.T,
        (1.0 / attn_gain)[:, None],
        outer_product_gain[:, None],
        jnp.concatenate([w_left, w_right], 1).T,
        bias,
        mask,
    )
    gated, left, right = made[:ROWS], made[ROWS], made[ROWS + 1]

    left = lax.ppermute(left, ("row", "col"), SCATTER)
    along_z = jnp.concatenate([left] + [lax.ppermute(left, "col", shift_z(n)) for n in range(1, 4)], 0)
    rights = [right] + [lax.ppermute(right, "row", shift(ROWS, n)) for n in range(1, ROWS)]
    along_x = [along_z] + [lax.ppermute(along_z, "col", shift_x(n)) for n in range(1, 4)]
    lefts = along_x + [lax.ppermute(part, "col", SWAP) for part in along_x]
    returned = [gated[0]] + [lax.ppermute(gated[n], "row", shift(ROWS, n)) for n in range(1, ROWS)]

    depth, across, core = col // 8, col // 2 % 4, col % 2
    scalars = jnp.stack(
        [row]
        + [
            (depth - n) % 4 * 8 + (across - m) % 4 * 2 + side
            for side in (core, 1 - core)
            for m in range(4)
            for n in range(4)
        ]
    ).astype(jnp.int32)
    rows_live = lax.dynamic_slice_in_dim(res_mask, row * PAIR_ROWS, PAIR_ROWS, 0)
    inverse = 1.0 / jnp.maximum(jnp.sum(seq_mask) * own_res, 1).astype(F32)
    pair = pl.pallas_call(
        pair_kernel,
        out_shape=jax.ShapeDtypeStruct((PAIR_ROWS, RES, CZ), F32),
        in_specs=[SMEM] * 2 + [VMEM] * (3 + ROWS + len(lefts)),
        out_specs=VMEM,
        scratch_shapes=[
            pltpu.VMEM((PAIR_ROWS * COPM, TOTAL), BF),
            pltpu.VMEM((RES * COPM, TOTAL), BF),
            pltpu.VMEM((RES * COPM, TOTAL), BF),
            pltpu.VMEM((PAIR_ROWS // GROUP * RES, COPM * GROUP * COPM), BF),
        ],
        name="pair",
    )(scalars, rows_live, ORDER, jnp.broadcast_to(inverse[:, None], (RES, CZ)), wide, *rights, *lefts)
    added = pl.pallas_call(
        add_kernel,
        out_shape=jax.ShapeDtypeStruct((SEQ * RES, C), F32),
        in_specs=[SMEM] + [VMEM] * (2 + ROWS),
        out_specs=VMEM,
        scratch_shapes=[pltpu.VMEM((SEQ * RES, 128), F32)] * 2,
        name="add",
    )(rank, tokens, output_weight, *returned)
    return added.reshape(SEQ, RES, C), pair


def solution(mesh):
    in_specs = (P("row", "col", None),) + (P(),) * 12
    out_specs = (P("row", "col", None), P("row", "col", None))
    return jax.shard_map(shards, mesh=mesh, in_specs=in_specs, out_specs=out_specs, check_vma=False)
```

```python
import functools

import jax
import jax.numpy as jnp
import numpy as np
from jax import lax
from jax.experimental import pallas as pl
from jax.experimental.pallas import tpu as pltpu
from jax.sharding import PartitionSpec as P


HEADS = 8
HEAD_DIM = 32
ROWS = 8
COLS = 32
SEQ = 64
RES = 24
OWN = RES // ROWS
TOTAL = SEQ * ROWS
PAIR_ROWS = RES * COLS // ROWS
BLOCK = OWN * SEQ
GROUP = 4
SIDE = OWN * 32
PIECES = 16
MIB = 1 << 20
C = 256
COPM = 32
CZ = 128
EPS = 1e-05
BF = jnp.bfloat16
F32 = jnp.float32
VMEM = pl.BlockSpec(memory_space=pltpu.VMEM)
SMEM = pl.BlockSpec(memory_space=pltpu.SMEM)
ANY = pl.BlockSpec(memory_space=pl.ANY)


def dot(a, b):
    return jnp.dot(a, b, preferred_element_type=F32)


def iota(shape, dim):
    return lax.broadcasted_iota(jnp.int32, shape, dim)


def column(values):
    return jnp.broadcast_to(values, (8, values.shape[1])).T[:, 0:1]


def norm_kernel(place_ref, align_ref, gain_ref, *refs):
    outs, halves = refs[:ROWS], refs[ROWS:]
    for i in range(2):
        halves[i][...] = align_ref[:, i * 128 : (i + 1) * 128]
    rank = place_ref[0]
    gain = gain_ref[...]
    row = iota((SEQ, 128), 0)
    lane = iota((SEQ, 128), 1)
    row16 = iota((16, 128), 0)
    for n in range(ROWS):
        first = lax.rem(rank + n, ROWS) * OWN
        extra = jnp.zeros((16, 128), F32)
        for j in range(OWN):
            x = jnp.concatenate([half[pl.ds(first + j, SEQ, stride=RES), :] for half in halves], 1)
            centred = x - jnp.mean(x, -1, keepdims=True)
            spread = jnp.mean(centred * centred, -1, keepdims=True) + EPS
            normed = centred * lax.rsqrt(spread) * gain
            outs[n][j * SEQ : (j + 1) * SEQ, :] = normed.astype(BF)
            sigma = jnp.sqrt(spread)
            high = sigma.astype(BF).astype(F32)
            low = sigma - high
            spots = jnp.where(lane == row, high, jnp.where(lane == row + SEQ, low, 0.0))
            extra = extra + jnp.where(row16 == j, jnp.sum(spots, 0, keepdims=True), 0.0)
        outs[n][BLOCK : BLOCK + 16, 0:128] = extra.astype(BF)
        outs[n][BLOCK : BLOCK + 16, 128:256] = jnp.zeros((16, 128), BF)


def attend_kernel(*refs):
    place_ref, res_mask_ref = refs[:2]
    blocks = refs[2:10]
    (wq_ref, wk_ref, wv_ref, wg_ref, wo_ref, gain_ref, gain2_ref, wl_ref, wr_ref, mask_ref) = refs[10:20]
    back_ref, left_ref, rights_ref, gated_ref, gate_ref = refs[20:]
    rank = place_ref[0]
    first_res = place_ref[1] * RES + rank * OWN
    seen = jnp.broadcast_to(mask_ref[...].astype(F32), (8, TOTAL))
    seen = pltpu.roll(seen, lax.rem(ROWS - rank, ROWS) * SEQ, 1)[0:1]
    bias = column(jnp.where(seen > 0, 0.0, -1000000000.0))
    inv_gain = column(1.0 / gain_ref[...])
    gain2 = column(gain2_ref[...])
    wq, wv, wg, wo = (ref[...].T for ref in (wq_ref, wv_ref, wg_ref, wo_ref))
    wlr = jnp.concatenate([wl_ref[...].astype(F32), wr_ref[...].astype(F32)], 1).T.astype(BF)
    lane_head = iota((1, C), 1) // HEAD_DIM
    half = iota((1, 128), 1) < SEQ
    for j in range(OWN):
        x = jnp.concatenate([b[j * SEQ : (j + 1) * SEQ, :] for b in blocks], 0)
        xt = x.T
        keys = dot(x, wk_ref[...]).astype(BF)
        qt = (dot(wq, xt) * HEAD_DIM**-0.5).astype(BF)
        vt = dot(wv, xt).astype(BF)
        gate_ref[...] = jax.nn.sigmoid(dot(wg, xt))
        for h in range(HEADS):
            own = slice(h * HEAD_DIM, (h + 1) * HEAD_DIM)
            head_keys = keys * (lane_head == h).astype(BF)
            for s in range(TOTAL // C):
                cols = slice(s * C, (s + 1) * C)
                logits = dot(head_keys, qt[:, cols]) + bias
                top = jnp.max(logits, 0, keepdims=True)
                weights = jnp.exp(logits - top)
                total = jnp.sum(weights, 0, keepdims=True)
                mixed = dot(vt[own, :], weights.astype(BF)) / total
                gated_ref[own, cols] = (mixed * gate_ref[own, cols]).astype(BF)
        gated = gated_ref[...]
        rows = gated.T
        for p in range(ROWS):
            back_ref[lax.rem(rank + p, ROWS), j * SEQ : (j + 1) * SEQ, :] = rows[p * SEQ : (p + 1) * SEQ, :]
        pieces = []
        for p in range(0, ROWS, 2):
            tiles = []
            for b in blocks[p : p + 2]:
                tile = b[BLOCK : BLOCK + 16, 0:128].astype(F32)[j : j + 1]
                tiles.append(tile + pltpu.roll(tile, SEQ, 1))
            pieces.append(jnp.where(half, tiles[0], tiles[1]))
        sigma = jnp.concatenate(pieces, 1)
        y = dot(wo, gated) + xt.astype(F32) * inv_gain * sigma
        centred = y - jnp.mean(y, 0, keepdims=True)
        spread = jnp.mean(centred * centred, 0, keepdims=True)
        second = (centred * lax.rsqrt(spread + EPS) * gain2).astype(BF)
        live = res_mask_ref[first_res + j].astype(F32)
        sides = dot(wlr, second) * (seen * live)
        sides = pltpu.roll(sides, rank * SEQ, 1).astype(BF)
        left_ref[j * COPM : (j + 1) * COPM, :] = sides[:COPM]
        for p in range(ROWS):
            rights_ref[p, j * COPM : (j + 1) * COPM, :] = sides[COPM:]


def add_kernel(align_ref, wo_ref, back_ref, out_ref, *halves):
    for n in range(ROWS):
        delta = dot(back_ref[n], wo_ref[...])
        for j in range(OWN):
            for i in range(2):
                part = delta[j * SEQ : (j + 1) * SEQ, i * 128 : (i + 1) * 128]
                halves[i][pl.ds(n * OWN + j, SEQ, stride=RES), :] = part
    for i in range(2):
        lanes = slice(i * 128, (i + 1) * 128)
        out_ref[:, lanes] = align_ref[:, lanes] + halves[i][...]


def widen_kernel(w_ref, out_ref, wide_ref):
    wide_ref[...] = w_ref[...].astype(F32)
    out_ref[...] = jnp.zeros(out_ref.shape, BF)
    for b in range(COPM):
        part = wide_ref[pl.ds(b, COPM, stride=COPM), :].astype(BF)
        for i in range(GROUP):
            start = b * GROUP * COPM + i * COPM
            out_ref[start : start + COPM, i * CZ : (i + 1) * CZ] = part


def order_kernel(order_ref, rights_ref, out_ref):
    pick = (order_ref[...] == iota((RES * COPM, RES * COPM), 1)).astype(BF)
    out_ref[...] = dot(pick, rights_ref[...]).astype(BF)


def stack_kernel(*refs):
    parts, out_ref, sems = refs[:PIECES], refs[PIECES], refs[PIECES + 1]
    copies = [
        pltpu.make_async_copy(part, out_ref.at[n * SIDE : (n + 1) * SIDE, :], sems.at[n])
        for n, part in enumerate(parts)
    ]
    for copy in copies:
        copy.start()
    for copy in copies:
        copy.wait()


def pair_kernel(core, place_ref, res_mask_ref, mask_ref, wide_ref, right_ref, left_ref, *refs):
    out_ref, mid_ref, done_ref, out_sems = refs[-4:]
    row, col = place_ref[0], place_ref[1]
    total = jnp.sum(mask_ref[...].astype(F32), 1, keepdims=True)
    lines = iota((RES, CZ), 0)
    live = jnp.zeros((RES, CZ), F32)
    for j in range(RES):
        live = jnp.where(lines == j, res_mask_ref[col * RES + j].astype(F32), live)
    inverse = 1.0 / jnp.maximum(total * live, 1.0)
    depth, across = col // 8, lax.rem(col // 2, 4)
    side = lax.rem(col + core, 2)
    residues = []
    for n in range(PIECES):
        piece = lax.rem(depth + 4 - n % 4, 4) * 8 + lax.rem(across + 4 - n // 4, 4) * 2 + side
        residues.append(piece * OWN)
    for t in range(PIECES * SIDE // C):
        block = lax.dot_general(
            right_ref[...], left_ref[t * C : (t + 1) * C, :], (((1,), (1,)), ((), ())), preferred_element_type=F32
        )
        for b in range(COPM):
            rows = block[b * RES : (b + 1) * RES]
            mid_ref[t * 2 * RES : (t + 1) * 2 * RES, b * 128 : (b + 1) * 128] = jnp.concatenate(
                [rows[:, :128], rows[:, 128:]], 0
            ).astype(BF)
    for half in range(2):
        block = dot(mid_ref[...], wide_ref[:, half * C : (half + 1) * C])
        for t in range(PIECES * OWN // GROUP):
            for i in range(2):
                res = t * GROUP + half * 2 + i
                known = res_mask_ref[row * PAIR_ROWS + residues[res // OWN] + res % OWN]
                scale = jnp.where(known > 0, inverse, 1.0)
                done_ref[res] = block[t * RES : (t + 1) * RES, i * CZ : (i + 1) * CZ] * scale
    copies = [
        pltpu.make_async_copy(
            done_ref.at[n * OWN : (n + 1) * OWN], out_ref.at[pl.ds(residues[n], OWN)], out_sems.at[n]
        )
        for n in range(PIECES)
    ]
    for copy in copies:
        copy.start()
    for copy in copies:
        copy.wait()


def shift(n):
    return [(d, (d + n) % ROWS) for d in range(ROWS)]


def shift_z(n):
    return [(c, (c + 8 * n) % COLS) for c in range(COLS)]


def shift_x(n):
    return [(c, c // 8 * 8 + (c + 2 * n) % 8) for c in range(COLS)]


SWAP = [(c, c ^ 1) for c in range(COLS)]
SCATTER = [
    (r * COLS + c, c * ROWS // COLS * COLS + c % (COLS // ROWS) * ROWS + r) for r in range(ROWS) for c in range(COLS)
]
ORDER = np.array(
    [[j // OWN * SIDE + j % OWN * COPM + b] for b in range(COPM) for j in range(RES)], np.int32
)


def shards(
    alignment,
    seq_mask,
    res_mask,
    attn_gain,
    outer_product_gain,
    w_query,
    w_key,
    w_value,
    w_gate,
    output_weight,
    w_left,
    w_right,
    w_pair,
):
    place = jnp.stack([lax.axis_index("row"), lax.axis_index("col")]).astype(jnp.int32)
    tokens = alignment.reshape(SEQ * RES, C)
    mask = seq_mask[None]
    sent = pl.pallas_call(
        norm_kernel,
        out_shape=[jax.ShapeDtypeStruct((BLOCK + 16, C), BF)] * ROWS,
        in_specs=[SMEM, VMEM, VMEM],
        out_specs=[VMEM] * ROWS,
        scratch_shapes=[pltpu.VMEM((SEQ * RES, 128), F32)] * 2,
        compiler_params=pltpu.CompilerParams(vmem_limit_bytes=16 * MIB),
        name="norm",
    )(place, tokens, attn_gain[None])
    blocks = [sent[0]] + [None] * (ROWS - 1)
    for n in FIRST:
        blocks[ROWS - n] = lax.ppermute(sent[n], "row", shift(n))

    wide = pl.pallas_call(
        widen_kernel,
        out_shape=jax.ShapeDtypeStruct((COPM * GROUP * COPM, GROUP * CZ), BF),
        in_specs=[VMEM],
        out_specs=VMEM,
        scratch_shapes=[pltpu.VMEM((COPM * COPM, CZ), F32)],
        compiler_params=pltpu.CompilerParams(vmem_limit_bytes=16 * MIB),
        name="widen",
    )(w_pair)
    back, left, rights = pl.pallas_call(
        attend_kernel,
        out_shape=[
            jax.ShapeDtypeStruct((ROWS, BLOCK, C), BF),
            jax.ShapeDtypeStruct((SIDE, TOTAL), BF),
            jax.ShapeDtypeStruct((ROWS, SIDE, TOTAL), BF),
        ],
        in_specs=[SMEM] * 2 + [VMEM] * 18,
        out_specs=[VMEM] * 3,
        scratch_shapes=[pltpu.VMEM((C, TOTAL), BF), pltpu.VMEM((C, TOTAL), F32)],
        compiler_params=pltpu.CompilerParams(vmem_limit_bytes=24 * MIB),
        name="attend",
    )(
        place,
        res_mask,
        *blocks,
        w_query,
        w_key,
        w_value,
        w_gate,
        output_weight,
        attn_gain[None],
        outer_product_gain[None],
        w_left,
        w_right,
        mask,
    )

    left = lax.ppermute(left, ("row", "col"), SCATTER)
    rights = exchanged(rights)
    along_z = [left] + [lax.ppermute(left, "col", shift_z(n)) for n in range(1, 4)]
    own = list(along_z)
    for m in range(1, 4):
        own += [lax.ppermute(along_z[n], "col", shift_x(m)) for n in range(4)]
    back = exchanged(back)
    own = pl.pallas_call(
        stack_kernel,
        out_shape=jax.ShapeDtypeStruct((PIECES * SIDE, TOTAL), BF),
        in_specs=[ANY] * PIECES,
        out_specs=ANY,
        scratch_shapes=[pltpu.SemaphoreType.DMA((PIECES,))],
        compiler_params=pltpu.CompilerParams(vmem_limit_bytes=8 * MIB),
        name="stack",
    )(*own)
    other = lax.ppermute(own, "col", SWAP)
    right_all = pl.pallas_call(
        order_kernel,
        out_shape=jax.ShapeDtypeStruct((RES * COPM, TOTAL), BF),
        in_specs=[VMEM] * 2,
        out_specs=VMEM,
        compiler_params=pltpu.CompilerParams(vmem_limit_bytes=16 * MIB),
        name="order",
    )(ORDER, rights.reshape(RES * COPM, TOTAL))
    pair = None
    for core, pieces in enumerate((own, other)):
        extra = [] if pair is None else [pair]
        pair = pl.pallas_call(
            functools.partial(pair_kernel, core),
            out_shape=jax.ShapeDtypeStruct((PAIR_ROWS, RES, CZ), F32),
            in_specs=[SMEM] * 2 + [VMEM] * 4 + [ANY] * len(extra),
            out_specs=ANY,
            scratch_shapes=[
                pltpu.VMEM((PIECES * OWN // GROUP * RES, COPM * GROUP * COPM), BF),
                pltpu.VMEM((PIECES * OWN, RES, CZ), F32),
                pltpu.SemaphoreType.DMA((PIECES,)),
            ],
            input_output_aliases={6: 0} if extra else {},
            compiler_params=pltpu.CompilerParams(vmem_limit_bytes=24 * MIB),
        )(place, res_mask, mask, wide, right_all, pieces, *extra)
    added = pl.pallas_call(
        add_kernel,
        out_shape=jax.ShapeDtypeStruct((SEQ * RES, C), F32),
        in_specs=[VMEM] * 3,
        out_specs=VMEM,
        scratch_shapes=[pltpu.VMEM((SEQ * RES, 128), F32)] * 2,
        compiler_params=pltpu.CompilerParams(vmem_limit_bytes=16 * MIB),
        name="add",
    )(tokens, output_weight, back)
    return added.reshape(SEQ, RES, C), pair


FIRST = (1, 7, 3, 5, 4, 2, 6)


def exchanged(values):
    return lax.all_to_all(values, "row", split_axis=0, concat_axis=0, tiled=True)


def solution(mesh):
    in_specs = (P("row", "col", None),) + (P(),) * 12
    out_specs = (P("row", "col", None), P("row", "col", None))

    def step(*args):
        return shards(*args)

    step = jax.shard_map(step, mesh=mesh, in_specs=in_specs, out_specs=out_specs, check_vma=False)
    return step
```

```python
import functools

import jax
import jax.numpy as jnp
import numpy as np
from jax import lax
from jax.experimental import pallas as pl
from jax.experimental.pallas import tpu as pltpu
from jax.sharding import PartitionSpec as P


HEADS = 8
HEAD_DIM = 32
ROWS = 8
COLS = 32
SEQ = 64
RES = 24
OWN = RES // ROWS
TOTAL = SEQ * ROWS
PAIR_ROWS = RES * COLS // ROWS
BLOCK = OWN * SEQ
GROUP = 4
SIDE = OWN * 32
PIECES = 16
MIB = 1 << 20
C = 256
COPM = 32
CZ = 128
EPS = 1e-05
BF = jnp.bfloat16
F32 = jnp.float32
VMEM = pl.BlockSpec(memory_space=pltpu.VMEM)
SMEM = pl.BlockSpec(memory_space=pltpu.SMEM)
ANY = pl.BlockSpec(memory_space=pl.ANY)


def dot(a, b):
    return jnp.dot(a, b, preferred_element_type=F32)


def iota(shape, dim):
    return lax.broadcasted_iota(jnp.int32, shape, dim)


def column(values):
    return jnp.broadcast_to(values, (8, values.shape[1])).T[:, 0:1]


def norm_kernel(place_ref, align_ref, gain_ref, *refs):
    outs, halves = refs[:ROWS], refs[ROWS:]
    for i in range(2):
        halves[i][...] = align_ref[:, i * 128 : (i + 1) * 128]
    rank = place_ref[0]
    gain = gain_ref[...]
    row = iota((SEQ, 128), 0)
    lane = iota((SEQ, 128), 1)
    row16 = iota((16, 128), 0)
    for n in range(ROWS):
        first = lax.rem(rank + n, ROWS) * OWN
        extra = jnp.zeros((16, 128), F32)
        for j in range(OWN):
            x = jnp.concatenate([half[pl.ds(first + j, SEQ, stride=RES), :] for half in halves], 1)
            centred = x - jnp.mean(x, -1, keepdims=True)
            spread = jnp.mean(centred * centred, -1, keepdims=True) + EPS
            normed = centred * lax.rsqrt(spread) * gain
            outs[n][j * SEQ : (j + 1) * SEQ, :] = normed.astype(BF)
            sigma = jnp.sqrt(spread)
            high = sigma.astype(BF).astype(F32)
            low = sigma - high
            spots = jnp.where(lane == row, high, jnp.where(lane == row + SEQ, low, 0.0))
            extra = extra + jnp.where(row16 == j, jnp.sum(spots, 0, keepdims=True), 0.0)
        outs[n][BLOCK : BLOCK + 16, 0:128] = extra.astype(BF)
        outs[n][BLOCK : BLOCK + 16, 128:256] = jnp.zeros((16, 128), BF)


def attend_kernel(*refs):
    place_ref, res_mask_ref = refs[:2]
    blocks = refs[2:10]
    (wq_ref, wk_ref, wv_ref, wg_ref, wo_ref, gain_ref, gain2_ref, wl_ref, wr_ref, mask_ref) = refs[10:20]
    back_ref, left_ref, rights_ref, gated_ref, gate_ref = refs[20:]
    rank = place_ref[0]
    first_res = place_ref[1] * RES + rank * OWN
    seen = jnp.broadcast_to(mask_ref[...].astype(F32), (8, TOTAL))
    seen = pltpu.roll(seen, lax.rem(ROWS - rank, ROWS) * SEQ, 1)[0:1]
    bias = column(jnp.where(seen > 0, 0.0, -1000000000.0))
    inv_gain = column(1.0 / gain_ref[...])
    gain2 = column(gain2_ref[...])
    wq, wv, wg, wo = (ref[...].T for ref in (wq_ref, wv_ref, wg_ref, wo_ref))
    wlr = jnp.concatenate([wl_ref[...].astype(F32), wr_ref[...].astype(F32)], 1).T.astype(BF)
    lane_head = iota((1, C), 1) // HEAD_DIM
    half = iota((1, 128), 1) < SEQ
    for j in range(OWN):
        x = jnp.concatenate([b[j * SEQ : (j + 1) * SEQ, :] for b in blocks], 0)
        xt = x.T
        keys = dot(x, wk_ref[...]).astype(BF)
        qt = (dot(wq, xt) * HEAD_DIM**-0.5).astype(BF)
        vt = dot(wv, xt).astype(BF)
        gate_ref[...] = jax.nn.sigmoid(dot(wg, xt))
        for h in range(HEADS):
            own = slice(h * HEAD_DIM, (h + 1) * HEAD_DIM)
            head_keys = keys * (lane_head == h).astype(BF)
            for s in range(TOTAL // C):
                cols = slice(s * C, (s + 1) * C)
                logits = dot(head_keys, qt[:, cols]) + bias
                top = jnp.max(logits, 0, keepdims=True)
                weights = jnp.exp(logits - top)
                total = jnp.sum(weights, 0, keepdims=True)
                mixed = dot(vt[own, :], weights.astype(BF)) / total
                gated_ref[own, cols] = (mixed * gate_ref[own, cols]).astype(BF)
        gated = gated_ref[...]
        rows = gated.T
        for p in range(ROWS):
            back_ref[lax.rem(rank + p, ROWS), j * SEQ : (j + 1) * SEQ, :] = rows[p * SEQ : (p + 1) * SEQ, :]
        pieces = []
        for p in range(0, ROWS, 2):
            tiles = []
            for b in blocks[p : p + 2]:
                tile = b[BLOCK : BLOCK + 16, 0:128].astype(F32)[j : j + 1]
                tiles.append(tile + pltpu.roll(tile, SEQ, 1))
            pieces.append(jnp.where(half, tiles[0], tiles[1]))
        sigma = jnp.concatenate(pieces, 1)
        y = dot(wo, gated) + xt.astype(F32) * inv_gain * sigma
        centred = y - jnp.mean(y, 0, keepdims=True)
        spread = jnp.mean(centred * centred, 0, keepdims=True)
        second = (centred * lax.rsqrt(spread + EPS) * gain2).astype(BF)
        live = res_mask_ref[first_res + j].astype(F32)
        sides = dot(wlr, second) * (seen * live)
        sides = pltpu.roll(sides, rank * SEQ, 1).astype(BF)
        left_ref[j * COPM : (j + 1) * COPM, :] = sides[:COPM]
        for p in range(ROWS):
            rights_ref[p, j * COPM : (j + 1) * COPM, :] = sides[COPM:]


def add_kernel(align_ref, wo_ref, back_ref, out_ref, *halves):
    for n in range(ROWS):
        delta = dot(back_ref[n], wo_ref[...])
        for j in range(OWN):
            for i in range(2):
                part = delta[j * SEQ : (j + 1) * SEQ, i * 128 : (i + 1) * 128]
                halves[i][pl.ds(n * OWN + j, SEQ, stride=RES), :] = part
    for i in range(2):
        lanes = slice(i * 128, (i + 1) * 128)
        out_ref[:, lanes] = align_ref[:, lanes] + halves[i][...]


def widen_kernel(w_ref, out_ref, wide_ref):
    wide_ref[...] = w_ref[...].astype(F32)
    out_ref[...] = jnp.zeros(out_ref.shape, BF)
    for b in range(COPM):
        part = wide_ref[pl.ds(b, COPM, stride=COPM), :].astype(BF)
        for i in range(GROUP):
            start = b * GROUP * COPM + i * COPM
            out_ref[start : start + COPM, i * CZ : (i + 1) * CZ] = part


def order_kernel(order_ref, rights_ref, out_ref):
    pick = (order_ref[...] == iota((RES * COPM, RES * COPM), 1)).astype(BF)
    out_ref[...] = dot(pick, rights_ref[...]).astype(BF)


def pair_kernel(core, place_ref, res_mask_ref, mask_ref, wide_ref, right_ref, *refs):
    if core:
        left_ref, _, out_ref, mid_ref, done_ref, out_sems = refs
    else:
        lefts = refs[:PIECES]
        out_ref, stack_ref, mid_ref, done_ref, out_sems, left_ref, in_sems, stack_sem = refs[PIECES:]
        gathers = [
            pltpu.make_async_copy(left, left_ref.at[n * SIDE : (n + 1) * SIDE, :], in_sems.at[n])
            for n, left in enumerate(lefts)
        ]
        for copy in gathers:
            copy.start()
    row, col = place_ref[0], place_ref[1]
    total = jnp.sum(mask_ref[...].astype(F32), 1, keepdims=True)
    lines = iota((RES, CZ), 0)
    live = jnp.zeros((RES, CZ), F32)
    for j in range(RES):
        live = jnp.where(lines == j, res_mask_ref[col * RES + j].astype(F32), live)
    inverse = 1.0 / jnp.maximum(total * live, 1.0)
    depth, across = col // 8, lax.rem(col // 2, 4)
    side = lax.rem(col + core, 2)
    residues = []
    for n in range(PIECES):
        place_x = lax.rem(across + 8 - n // 4 - 2 * lax.rem(row, 2), 4)
        far = lax.rem(place_x + 1, 4) // 2
        source = place_x // 2 * 4 + lax.rem(depth + 4 - n % 4, 4)
        residues.append((2 * far + side) * RES + source * OWN)
    if not core:
        for copy in gathers:
            copy.wait()
        stacking = pltpu.make_async_copy(left_ref, stack_ref, stack_sem)
        stacking.start()
    for t in range(PIECES * SIDE // C):
        block = lax.dot_general(
            right_ref[...], left_ref[t * C : (t + 1) * C, :], (((1,), (1,)), ((), ())), preferred_element_type=F32
        )
        for b in range(COPM):
            rows = block[b * RES : (b + 1) * RES]
            mid_ref[t * 2 * RES : (t + 1) * 2 * RES, b * 128 : (b + 1) * 128] = jnp.concatenate(
                [rows[:, :128], rows[:, 128:]], 0
            ).astype(BF)
    for half in range(2):
        block = dot(mid_ref[...], wide_ref[:, half * C : (half + 1) * C])
        for t in range(PIECES * OWN // GROUP):
            for i in range(2):
                res = t * GROUP + half * 2 + i
                known = res_mask_ref[row * PAIR_ROWS + residues[res // OWN] + res % OWN]
                scale = jnp.where(known > 0, inverse, 1.0)
                done_ref[res] = block[t * RES : (t + 1) * RES, i * CZ : (i + 1) * CZ] * scale
    copies = [
        pltpu.make_async_copy(
            done_ref.at[n * OWN : (n + 1) * OWN], out_ref.at[pl.ds(residues[n], OWN)], out_sems.at[n]
        )
        for n in range(PIECES)
    ]
    for copy in copies:
        copy.start()
    for copy in copies:
        copy.wait()
    if not core:
        stacking.wait()


def shift(n):
    return [(d, (d + n) % ROWS) for d in range(ROWS)]


def shift_x(n):
    return [(c, c // 8 * 8 + (c + 2 * n) % 8) for c in range(COLS)]


SWAP = [(c, c ^ 1) for c in range(COLS)]


def scatter(depth):
    pairs = []
    for r in range(ROWS):
        for c in range(COLS):
            block, far, core = c // 4, c // 2 % 2, c % 2
            across = (2 * (block % 2) + far + (r // 4 if far else -(r // 4))) % 4
            pairs.append((r * COLS + c, block * COLS + (r + depth) % 4 * 8 + across * 2 + core))
    return pairs


ORDER = np.array(
    [[j // OWN * SIDE + j % OWN * COPM + b] for b in range(COPM) for j in range(RES)], np.int32
)


def shards(
    alignment,
    seq_mask,
    res_mask,
    attn_gain,
    outer_product_gain,
    w_query,
    w_key,
    w_value,
    w_gate,
    output_weight,
    w_left,
    w_right,
    w_pair,
):
    place = jnp.stack([lax.axis_index("row"), lax.axis_index("col")]).astype(jnp.int32)
    tokens = alignment.reshape(SEQ * RES, C)
    mask = seq_mask[None]
    sent = pl.pallas_call(
        norm_kernel,
        out_shape=[jax.ShapeDtypeStruct((BLOCK + 16, C), BF)] * ROWS,
        in_specs=[SMEM, VMEM, VMEM],
        out_specs=[VMEM] * ROWS,
        scratch_shapes=[pltpu.VMEM((SEQ * RES, 128), F32)] * 2,
        compiler_params=pltpu.CompilerParams(vmem_limit_bytes=16 * MIB),
        name="norm",
    )(place, tokens, attn_gain[None])
    blocks = [sent[0]] + [None] * (ROWS - 1)
    for n in FIRST:
        blocks[ROWS - n] = lax.ppermute(sent[n], "row", shift(n))

    wide = pl.pallas_call(
        widen_kernel,
        out_shape=jax.ShapeDtypeStruct((COPM * GROUP * COPM, GROUP * CZ), BF),
        in_specs=[VMEM],
        out_specs=VMEM,
        scratch_shapes=[pltpu.VMEM((COPM * COPM, CZ), F32)],
        compiler_params=pltpu.CompilerParams(vmem_limit_bytes=16 * MIB),
        name="widen",
    )(w_pair)
    back, left, rights = pl.pallas_call(
        attend_kernel,
        out_shape=[
            jax.ShapeDtypeStruct((ROWS, BLOCK, C), BF),
            jax.ShapeDtypeStruct((SIDE, TOTAL), BF),
            jax.ShapeDtypeStruct((ROWS, SIDE, TOTAL), BF),
        ],
        in_specs=[SMEM] * 2 + [VMEM] * 18,
        out_specs=[VMEM] * 3,
        scratch_shapes=[pltpu.VMEM((C, TOTAL), BF), pltpu.VMEM((C, TOTAL), F32)],
        compiler_params=pltpu.CompilerParams(vmem_limit_bytes=24 * MIB),
        name="attend",
    )(
        place,
        res_mask,
        *blocks,
        w_query,
        w_key,
        w_value,
        w_gate,
        output_weight,
        attn_gain[None],
        outer_product_gain[None],
        w_left,
        w_right,
        mask,
    )

    rights = exchanged(rights)
    along_z = [lax.ppermute(left, ("row", "col"), scatter(n)) for n in range(4)]
    own = list(along_z)
    for m in range(1, 4):
        own += [lax.ppermute(along_z[n], "col", shift_x(m)) for n in range(4)]
    back = exchanged(back)
    right_all = pl.pallas_call(
        order_kernel,
        out_shape=jax.ShapeDtypeStruct((RES * COPM, TOTAL), BF),
        in_specs=[VMEM] * 2,
        out_specs=VMEM,
        compiler_params=pltpu.CompilerParams(vmem_limit_bytes=16 * MIB),
        name="order",
    )(ORDER, rights.reshape(RES * COPM, TOTAL))
    shape = jax.ShapeDtypeStruct((PAIR_ROWS, RES, CZ), F32)
    stack_shape = jax.ShapeDtypeStruct((PIECES * SIDE, TOTAL), BF)
    scratch = [
        pltpu.VMEM((PIECES * OWN // GROUP * RES, COPM * GROUP * COPM), BF),
        pltpu.VMEM((PIECES * OWN, RES, CZ), F32),
        pltpu.SemaphoreType.DMA((PIECES,)),
    ]
    pair, stack = pl.pallas_call(
        functools.partial(pair_kernel, 0),
        out_shape=[shape, stack_shape],
        in_specs=[SMEM] * 2 + [VMEM] * 3 + [ANY] * PIECES,
        out_specs=[ANY, ANY],
        scratch_shapes=scratch
        + [
            pltpu.VMEM((PIECES * SIDE, TOTAL), BF),
            pltpu.SemaphoreType.DMA((PIECES,)),
            pltpu.SemaphoreType.DMA,
        ],
        compiler_params=pltpu.CompilerParams(vmem_limit_bytes=24 * MIB),
        name="pair0",
    )(place, res_mask, mask, wide, right_all, *own)
    other = lax.ppermute(stack, "col", SWAP)
    pair = pl.pallas_call(
        functools.partial(pair_kernel, 1),
        out_shape=shape,
        in_specs=[SMEM] * 2 + [VMEM] * 4 + [ANY],
        out_specs=ANY,
        scratch_shapes=scratch,
        input_output_aliases={6: 0},
        compiler_params=pltpu.CompilerParams(vmem_limit_bytes=24 * MIB),
        name="pair1",
    )(place, res_mask, mask, wide, right_all, other, pair)
    added = pl.pallas_call(
        add_kernel,
        out_shape=jax.ShapeDtypeStruct((SEQ * RES, C), F32),
        in_specs=[VMEM] * 3,
        out_specs=VMEM,
        scratch_shapes=[pltpu.VMEM((SEQ * RES, 128), F32)] * 2,
        compiler_params=pltpu.CompilerParams(vmem_limit_bytes=16 * MIB),
        name="add",
    )(tokens, output_weight, back)
    return added.reshape(SEQ, RES, C), pair


FIRST = (1, 7, 3, 5, 4, 2, 6)


def exchanged(values):
    return lax.all_to_all(values, "row", split_axis=0, concat_axis=0, tiled=True)


def solution(mesh):
    in_specs = (P("row", "col", None),) + (P(),) * 12
    out_specs = (P("row", "col", None), P("row", "col", None))

    def step(*args):
        return shards(*args)

    step = jax.shard_map(step, mesh=mesh, in_specs=in_specs, out_specs=out_specs, check_vma=False)
    return step
```

```python
import functools

import jax
import jax.numpy as jnp
import numpy as np
from jax import lax
from jax.experimental import pallas as pl
from jax.experimental.pallas import tpu as pltpu
from jax.sharding import PartitionSpec as P


HEADS = 8
HEAD_DIM = 32
ROWS = 8
COLS = 32
SEQ = 64
RES = 24
OWN = RES // ROWS
TOTAL = SEQ * ROWS
PAIR_ROWS = RES * COLS // ROWS
BLOCK = OWN * SEQ
GROUP = 4
SIDE = OWN * 32
QUARTER = 4 * SIDE
MIB = 1 << 20
C = 256
COPM = 32
CZ = 128
EPS = 1e-05
BF = jnp.bfloat16
F32 = jnp.float32
VMEM = pl.BlockSpec(memory_space=pltpu.VMEM)
SMEM = pl.BlockSpec(memory_space=pltpu.SMEM)
ANY = pl.BlockSpec(memory_space=pl.ANY)


def dot(a, b):
    return jnp.dot(a, b, preferred_element_type=F32)


def iota(shape, dim):
    return lax.broadcasted_iota(jnp.int32, shape, dim)


def column(values):
    return jnp.broadcast_to(values, (8, values.shape[1])).T[:, 0:1]


def norm_kernel(place_ref, align_ref, gain_ref, *refs):
    outs, halves = refs[:ROWS], refs[ROWS:]
    for i in range(2):
        halves[i][...] = align_ref[:, i * 128 : (i + 1) * 128]
    rank = place_ref[0]
    gain = gain_ref[...]
    row = iota((SEQ, 128), 0)
    lane = iota((SEQ, 128), 1)
    row16 = iota((16, 128), 0)
    for n in range(ROWS):
        first = lax.rem(rank + n, ROWS) * OWN
        extra = jnp.zeros((16, 128), F32)
        for j in range(OWN):
            x = jnp.concatenate([half[pl.ds(first + j, SEQ, stride=RES), :] for half in halves], 1)
            centred = x - jnp.mean(x, -1, keepdims=True)
            spread = jnp.mean(centred * centred, -1, keepdims=True) + EPS
            normed = centred * lax.rsqrt(spread) * gain
            outs[n][j * SEQ : (j + 1) * SEQ, :] = normed.astype(BF)
            sigma = jnp.sqrt(spread)
            high = sigma.astype(BF).astype(F32)
            low = sigma - high
            spots = jnp.where(lane == row, high, jnp.where(lane == row + SEQ, low, 0.0))
            extra = extra + jnp.where(row16 == j, jnp.sum(spots, 0, keepdims=True), 0.0)
        outs[n][BLOCK : BLOCK + 16, 0:128] = extra.astype(BF)
        outs[n][BLOCK : BLOCK + 16, 128:256] = jnp.zeros((16, 128), BF)


def attend_kernel(*refs):
    place_ref, res_mask_ref = refs[:2]
    blocks = refs[2:10]
    (wq_ref, wk_ref, wv_ref, wg_ref, wo_ref, gain_ref, gain2_ref, wl_ref, wr_ref, mask_ref) = refs[10:20]
    back_ref, left_ref, rights_ref, gated_ref, gate_ref = refs[20:]
    rank = place_ref[0]
    first_res = place_ref[1] * RES + rank * OWN
    seen = jnp.broadcast_to(mask_ref[...].astype(F32), (8, TOTAL))
    seen = pltpu.roll(seen, lax.rem(ROWS - rank, ROWS) * SEQ, 1)[0:1]
    bias = column(jnp.where(seen > 0, 0.0, -1000000000.0))
    inv_gain = column(1.0 / gain_ref[...])
    gain2 = column(gain2_ref[...])
    wq, wv, wg, wo = (ref[...].T for ref in (wq_ref, wv_ref, wg_ref, wo_ref))
    wlr = jnp.concatenate([wl_ref[...].astype(F32), wr_ref[...].astype(F32)], 1).T.astype(BF)
    lane_head = iota((1, C), 1) // HEAD_DIM
    half = iota((1, 128), 1) < SEQ
    for j in range(OWN):
        x = jnp.concatenate([b[j * SEQ : (j + 1) * SEQ, :] for b in blocks], 0)
        xt = x.T
        keys = dot(x, wk_ref[...]).astype(BF)
        qt = (dot(wq, xt) * HEAD_DIM**-0.5).astype(BF)
        vt = dot(wv, xt).astype(BF)
        gate_ref[...] = jax.nn.sigmoid(dot(wg, xt))
        for h in range(HEADS):
            own = slice(h * HEAD_DIM, (h + 1) * HEAD_DIM)
            head_keys = keys * (lane_head == h).astype(BF)
            for s in range(TOTAL // C):
                cols = slice(s * C, (s + 1) * C)
                logits = dot(head_keys, qt[:, cols]) + bias
                top = jnp.max(logits, 0, keepdims=True)
                weights = jnp.exp(logits - top)
                total = jnp.sum(weights, 0, keepdims=True)
                mixed = dot(vt[own, :], weights.astype(BF)) / total
                gated_ref[own, cols] = (mixed * gate_ref[own, cols]).astype(BF)
        gated = gated_ref[...]
        rows = gated.T
        for p in range(ROWS):
            back_ref[lax.rem(rank + p, ROWS), j * SEQ : (j + 1) * SEQ, :] = rows[p * SEQ : (p + 1) * SEQ, :]
        pieces = []
        for p in range(0, ROWS, 2):
            tiles = []
            for b in blocks[p : p + 2]:
                tile = b[BLOCK : BLOCK + 16, 0:128].astype(F32)[j : j + 1]
                tiles.append(tile + pltpu.roll(tile, SEQ, 1))
            pieces.append(jnp.where(half, tiles[0], tiles[1]))
        sigma = jnp.concatenate(pieces, 1)
        y = dot(wo, gated) + xt.astype(F32) * inv_gain * sigma
        centred = y - jnp.mean(y, 0, keepdims=True)
        spread = jnp.mean(centred * centred, 0, keepdims=True)
        second = (centred * lax.rsqrt(spread + EPS) * gain2).astype(BF)
        live = res_mask_ref[first_res + j].astype(F32)
        sides = dot(wlr, second) * (seen * live)
        sides = pltpu.roll(sides, rank * SEQ, 1).astype(BF)
        left_ref[j * COPM : (j + 1) * COPM, :] = sides[:COPM]
        for p in range(ROWS):
            rights_ref[p, j * COPM : (j + 1) * COPM, :] = sides[COPM:]


def add_kernel(align_ref, wo_ref, back_ref, out_ref, *halves):
    for n in range(ROWS):
        delta = dot(back_ref[n], wo_ref[...])
        for j in range(OWN):
            for i in range(2):
                part = delta[j * SEQ : (j + 1) * SEQ, i * 128 : (i + 1) * 128]
                halves[i][pl.ds(n * OWN + j, SEQ, stride=RES), :] = part
    for i in range(2):
        lanes = slice(i * 128, (i + 1) * 128)
        out_ref[:, lanes] = align_ref[:, lanes] + halves[i][...]


def widen_kernel(w_ref, out_ref, wide_ref):
    wide_ref[...] = w_ref[...].astype(F32)
    out_ref[...] = jnp.zeros(out_ref.shape, BF)
    for b in range(COPM):
        part = wide_ref[pl.ds(b, COPM, stride=COPM), :].astype(BF)
        for i in range(GROUP):
            start = b * GROUP * COPM + i * COPM
            out_ref[start : start + COPM, i * CZ : (i + 1) * CZ] = part


def order_kernel(order_ref, rights_ref, out_ref):
    pick = (order_ref[...] == iota((RES * COPM, RES * COPM), 1)).astype(BF)
    out_ref[...] = dot(pick, rights_ref[...]).astype(BF)


def pair_kernel(quarters, place_ref, res_mask_ref, mask_ref, wide_ref, right_ref, *refs):
    count = len(quarters)
    lefts = refs[:count]
    out_ref, left_ref, mid_ref, done_ref, in_sems, out_sems = refs[-6:]
    gathers = [
        pltpu.make_async_copy(left, left_ref.at[n * QUARTER : (n + 1) * QUARTER, :], in_sems.at[n])
        for n, left in enumerate(lefts)
    ]
    for copy in gathers:
        copy.start()
    row, col = place_ref[0], place_ref[1]
    total = jnp.sum(mask_ref[...].astype(F32), 1, keepdims=True)
    lines = iota((RES, CZ), 0)
    live = jnp.zeros((RES, CZ), F32)
    for j in range(RES):
        live = jnp.where(lines == j, res_mask_ref[col * RES + j].astype(F32), live)
    inverse = 1.0 / jnp.maximum(total * live, 1.0)
    depth, across = col // 8, lax.rem(col // 2, 4)
    residues = []
    for shifted, other in quarters:
        side = lax.rem(col + other, 2)
        place_x = lax.rem(across + 8 - shifted - 2 * lax.rem(row, 2), 4)
        far = lax.rem(place_x + 1, 4) // 2
        for n in range(4):
            source = place_x // 2 * 4 + lax.rem(depth + 4 - n, 4)
            residues.append((2 * far + side) * RES + source * OWN)
    for copy in gathers:
        copy.wait()
    for t in range(count * QUARTER // C):
        block = lax.dot_general(
            right_ref[...], left_ref[t * C : (t + 1) * C, :], (((1,), (1,)), ((), ())), preferred_element_type=F32
        )
        for b in range(COPM):
            rows = block[b * RES : (b + 1) * RES]
            mid_ref[t * 2 * RES : (t + 1) * 2 * RES, b * 128 : (b + 1) * 128] = jnp.concatenate(
                [rows[:, :128], rows[:, 128:]], 0
            ).astype(BF)
    for half in range(2):
        block = dot(mid_ref[...], wide_ref[:, half * C : (half + 1) * C])
        for t in range(len(residues) * OWN // GROUP):
            for i in range(2):
                res = t * GROUP + half * 2 + i
                known = res_mask_ref[row * PAIR_ROWS + residues[res // OWN] + res % OWN]
                scale = jnp.where(known > 0, inverse, 1.0)
                done_ref[res] = block[t * RES : (t + 1) * RES, i * CZ : (i + 1) * CZ] * scale
    copies = [
        pltpu.make_async_copy(
            done_ref.at[n * OWN : (n + 1) * OWN], out_ref.at[pl.ds(residues[n], OWN)], out_sems.at[n]
        )
        for n in range(len(residues))
    ]
    for copy in copies:
        copy.start()
    for copy in copies:
        copy.wait()


def shift(n):
    return [(d, (d + n) % ROWS) for d in range(ROWS)]


def shift_x(n):
    return [(c, c // 8 * 8 + (c + 2 * n) % 8) for c in range(COLS)]


SWAP = [(c, c ^ 1) for c in range(COLS)]


def scatter(depth):
    pairs = []
    for r in range(ROWS):
        for c in range(COLS):
            block, far, core = c // 4, c // 2 % 2, c % 2
            across = (2 * (block % 2) + far + (r // 4 if far else -(r // 4))) % 4
            pairs.append((r * COLS + c, block * COLS + (r + depth) % 4 * 8 + across * 2 + core))
    return pairs


ORDER = np.array(
    [[j // OWN * SIDE + j % OWN * COPM + b] for b in range(COPM) for j in range(RES)], np.int32
)


def shards(
    alignment,
    seq_mask,
    res_mask,
    attn_gain,
    outer_product_gain,
    w_query,
    w_key,
    w_value,
    w_gate,
    output_weight,
    w_left,
    w_right,
    w_pair,
):
    place = jnp.stack([lax.axis_index("row"), lax.axis_index("col")]).astype(jnp.int32)
    tokens = alignment.reshape(SEQ * RES, C)
    mask = seq_mask[None]
    sent = pl.pallas_call(
        norm_kernel,
        out_shape=[jax.ShapeDtypeStruct((BLOCK + 16, C), BF)] * ROWS,
        in_specs=[SMEM, VMEM, VMEM],
        out_specs=[VMEM] * ROWS,
        scratch_shapes=[pltpu.VMEM((SEQ * RES, 128), F32)] * 2,
        compiler_params=pltpu.CompilerParams(vmem_limit_bytes=16 * MIB),
        name="norm",
    )(place, tokens, attn_gain[None])
    blocks = [sent[0]] + [None] * (ROWS - 1)
    for n in FIRST:
        blocks[ROWS - n] = lax.ppermute(sent[n], "row", shift(n))

    wide = pl.pallas_call(
        widen_kernel,
        out_shape=jax.ShapeDtypeStruct((COPM * GROUP * COPM, GROUP * CZ), BF),
        in_specs=[VMEM],
        out_specs=VMEM,
        scratch_shapes=[pltpu.VMEM((COPM * COPM, CZ), F32)],
        compiler_params=pltpu.CompilerParams(vmem_limit_bytes=16 * MIB),
        name="widen",
    )(w_pair)
    back, left, rights = pl.pallas_call(
        attend_kernel,
        out_shape=[
            jax.ShapeDtypeStruct((ROWS, BLOCK, C), BF),
            jax.ShapeDtypeStruct((SIDE, TOTAL), BF),
            jax.ShapeDtypeStruct((ROWS, SIDE, TOTAL), BF),
        ],
        in_specs=[SMEM] * 2 + [VMEM] * 18,
        out_specs=[VMEM] * 3,
        scratch_shapes=[pltpu.VMEM((C, TOTAL), BF), pltpu.VMEM((C, TOTAL), F32)],
        compiler_params=pltpu.CompilerParams(vmem_limit_bytes=24 * MIB),
        name="attend",
    )(
        place,
        res_mask,
        *blocks,
        w_query,
        w_key,
        w_value,
        w_gate,
        output_weight,
        attn_gain[None],
        outer_product_gain[None],
        w_left,
        w_right,
        mask,
    )

    rights = exchanged(rights)
    along_z = [lax.ppermute(left, ("row", "col"), scatter(n)) for n in range(4)]
    own = {0: jnp.concatenate(along_z, 0)}
    for m in (1, 3, 2):
        own[m] = lax.ppermute(own[0], "col", shift_x(m))
    other = {m: lax.ppermute(own[m], "col", SWAP) for m in range(4)}
    back = exchanged(back)
    right_all = pl.pallas_call(
        order_kernel,
        out_shape=jax.ShapeDtypeStruct((RES * COPM, TOTAL), BF),
        in_specs=[VMEM] * 2,
        out_specs=VMEM,
        compiler_params=pltpu.CompilerParams(vmem_limit_bytes=16 * MIB),
        name="order",
    )(ORDER, rights.reshape(RES * COPM, TOTAL))
    pair = []
    for moves in ((0, 1, 3), (2,)):
        quarters = [(m, side) for m in moves for side in range(2)]
        count = len(quarters)
        pair = [
            pl.pallas_call(
                functools.partial(pair_kernel, quarters),
                out_shape=jax.ShapeDtypeStruct((PAIR_ROWS, RES, CZ), F32),
                in_specs=[SMEM] * 2 + [VMEM] * 3 + [ANY] * (count + len(pair)),
                out_specs=ANY,
                scratch_shapes=[
                    pltpu.VMEM((count * QUARTER, TOTAL), BF),
                    pltpu.VMEM((count * 3 * RES, COPM * GROUP * COPM), BF),
                    pltpu.VMEM((count * 4 * OWN, RES, CZ), F32),
                    pltpu.SemaphoreType.DMA((count,)),
                    pltpu.SemaphoreType.DMA((count * 4,)),
                ],
                input_output_aliases={5 + count: 0} if pair else {},
                compiler_params=pltpu.CompilerParams(vmem_limit_bytes=28 * MIB),
            )(place, res_mask, mask, wide, right_all, *((own, other)[side][m] for m, side in quarters), *pair)
        ]
    added = pl.pallas_call(
        add_kernel,
        out_shape=jax.ShapeDtypeStruct((SEQ * RES, C), F32),
        in_specs=[VMEM] * 3,
        out_specs=VMEM,
        scratch_shapes=[pltpu.VMEM((SEQ * RES, 128), F32)] * 2,
        compiler_params=pltpu.CompilerParams(vmem_limit_bytes=16 * MIB),
        name="add",
    )(tokens, output_weight, back)
    return added.reshape(SEQ, RES, C), pair[0]


FIRST = (1, 7, 3, 5, 4, 2, 6)


def exchanged(values):
    return lax.all_to_all(values, "row", split_axis=0, concat_axis=0, tiled=True)


def solution(mesh):
    in_specs = (P("row", "col", None),) + (P(),) * 12
    out_specs = (P("row", "col", None), P("row", "col", None))

    def step(*args):
        return shards(*args)

    step = jax.shard_map(step, mesh=mesh, in_specs=in_specs, out_specs=out_specs, check_vma=False)
    return step
```

```python
import functools

import jax
import jax.numpy as jnp
import numpy as np
from jax import lax
from jax.experimental import pallas as pl
from jax.experimental.pallas import tpu as pltpu
from jax.sharding import PartitionSpec as P


HEAD_DIM = 32
ROWS = 8
COLS = 32
SEQ = 64
RES = 24
OWN = RES // ROWS
TOTAL = SEQ * ROWS
PAIR_ROWS = RES * COLS // ROWS
BLOCK = OWN * SEQ
GROUP = 4
SIDE = OWN * 32
QUARTER = 4 * SIDE
MIB = 1 << 20
C = 256
COPM = 32
CZ = 128
EPS = 1e-05
BF = jnp.bfloat16
F32 = jnp.float32
VMEM = pl.BlockSpec(memory_space=pltpu.VMEM)
SMEM = pl.BlockSpec(memory_space=pltpu.SMEM)
ANY = pl.BlockSpec(memory_space=pl.ANY)


def dot(a, b):
    return jnp.dot(a, b, preferred_element_type=F32)


def iota(shape, dim):
    return lax.broadcasted_iota(jnp.int32, shape, dim)


def column(values):
    return jnp.broadcast_to(values, (8, values.shape[1])).T[:, 0:1]


def norm_kernel(place_ref, align_ref, gain_ref, *refs):
    outs, halves = refs[:ROWS], refs[ROWS:]
    for i in range(2):
        halves[i][...] = align_ref[:, i * 128 : (i + 1) * 128]
    rank = place_ref[0]
    gain = gain_ref[...]
    row = iota((SEQ, 128), 0)
    lane = iota((SEQ, 128), 1)
    row16 = iota((16, 128), 0)
    for n in range(ROWS):
        first = lax.rem(rank + n, ROWS) * OWN
        extra = jnp.zeros((16, 128), F32)
        for j in range(OWN):
            x = jnp.concatenate([half[pl.ds(first + j, SEQ, stride=RES), :] for half in halves], 1)
            centred = x - jnp.mean(x, -1, keepdims=True)
            spread = jnp.mean(centred * centred, -1, keepdims=True) + EPS
            normed = centred * lax.rsqrt(spread) * gain
            outs[n][j * SEQ : (j + 1) * SEQ, :] = normed.astype(BF)
            sigma = jnp.sqrt(spread)
            high = sigma.astype(BF).astype(F32)
            low = sigma - high
            spots = jnp.where(lane == row, high, jnp.where(lane == row + SEQ, low, 0.0))
            extra = extra + jnp.where(row16 == j, jnp.sum(spots, 0, keepdims=True), 0.0)
        outs[n][BLOCK : BLOCK + 16, 0:128] = extra.astype(BF)
        outs[n][BLOCK : BLOCK + 16, 128:256] = jnp.zeros((16, 128), BF)


def attend_kernel(*refs):
    place_ref, res_mask_ref = refs[:2]
    blocks = refs[2:10]
    (wq_ref, wk_ref, wv_ref, wg_ref, wo_ref, gain_ref, gain2_ref, wl_ref, wr_ref, mask_ref) = refs[10:20]
    out_ref, left_ref, gated_ref, gate_ref = refs[20:]
    rank = place_ref[0]
    first_res = place_ref[1] * RES + rank * OWN
    seen = jnp.broadcast_to(mask_ref[...].astype(F32), (8, TOTAL))
    seen = pltpu.roll(seen, lax.rem(ROWS - rank, ROWS) * SEQ, 1)[0:1]
    bias = jnp.where(seen > 0, 0.0, -1000000000.0)
    inv_gain = column(1.0 / gain_ref[...])
    gain2 = column(gain2_ref[...])
    wk, wo = wk_ref[...].T, wo_ref[...].T
    wlr = jnp.concatenate([wl_ref[...].astype(F32), wr_ref[...].astype(F32)], 1).T.astype(BF)
    lane_head = iota((1, C), 1) // HEAD_DIM
    half = iota((1, 128), 1) < SEQ
    tile_head = iota((TOTAL, 128), 1) // HEAD_DIM
    ones = jnp.ones((TOTAL, 128), BF)
    for j in range(OWN):
        x = jnp.concatenate([b[j * SEQ : (j + 1) * SEQ, :] for b in blocks], 0)
        xt = x.T
        queries = (dot(x, wq_ref[...]) * HEAD_DIM**-0.5).astype(BF)
        kt = dot(wk, xt).astype(BF)
        values = dot(x, wv_ref[...]).astype(BF)
        gate_ref[...] = jax.nn.sigmoid(dot(x, wg_ref[...]))
        for tile in range(C // 128):
            lanes = slice(tile * 128, (tile + 1) * 128)
            wide = jnp.concatenate([values[:, lanes], ones], 1)
            mixed = jnp.zeros((TOTAL, 128), F32)
            for h in range(128 // HEAD_DIM):
                picked = (lane_head == tile * (128 // HEAD_DIM) + h).astype(BF)
                logits = dot(queries * picked, kt) + bias
                top = jnp.max(logits, 1, keepdims=True)
                weights = jnp.exp(logits - top).astype(BF)
                both = dot(weights, wide)
                mixed = jnp.where(tile_head == h, both[:, :128] / both[:, 128:], mixed)
            gated_ref[:, lanes] = (mixed * gate_ref[:, lanes]).astype(BF)
        rows = gated_ref[...]
        gated = rows.T
        for p in range(ROWS):
            out_ref[lax.rem(rank + p, ROWS), j * SEQ : (j + 1) * SEQ, :] = rows[p * SEQ : (p + 1) * SEQ, :]
        pieces = []
        for p in range(0, ROWS, 2):
            tiles = []
            for b in blocks[p : p + 2]:
                tile = b[BLOCK : BLOCK + 16, 0:128].astype(F32)[j : j + 1]
                tiles.append(tile + pltpu.roll(tile, SEQ, 1))
            pieces.append(jnp.where(half, tiles[0], tiles[1]))
        sigma = jnp.concatenate(pieces, 1)
        y = dot(wo, gated) + xt.astype(F32) * inv_gain * sigma
        centred = y - jnp.mean(y, 0, keepdims=True)
        spread = jnp.mean(centred * centred, 0, keepdims=True)
        second = (centred * lax.rsqrt(spread + EPS) * gain2).astype(BF)
        live = res_mask_ref[first_res + j].astype(F32)
        sides = dot(wlr, second) * (seen * live)
        sides = pltpu.roll(sides, rank * SEQ, 1).astype(BF)
        left_ref[j * COPM : (j + 1) * COPM, :] = sides[:COPM]
        for p in range(ROWS):
            for i in range(2):
                spot = BLOCK + i * SIDE + j * COPM
                out_ref[p, spot : spot + COPM, :] = sides[COPM:, i * C : (i + 1) * C]


def add_kernel(align_ref, wo_ref, mixed_ref, out_ref, *halves):
    for n in range(ROWS):
        delta = dot(mixed_ref[n, 0:BLOCK, :], wo_ref[...])
        for j in range(OWN):
            for i in range(2):
                part = delta[j * SEQ : (j + 1) * SEQ, i * 128 : (i + 1) * 128]
                halves[i][pl.ds(n * OWN + j, SEQ, stride=RES), :] = part
    for i in range(2):
        lanes = slice(i * 128, (i + 1) * 128)
        out_ref[:, lanes] = align_ref[:, lanes] + halves[i][...]


def widen_kernel(w_ref, out_ref, wide_ref):
    wide_ref[...] = w_ref[...].astype(F32)
    out_ref[...] = jnp.zeros(out_ref.shape, BF)
    for b in range(COPM):
        part = wide_ref[pl.ds(b, COPM, stride=COPM), :].astype(BF)
        for i in range(GROUP):
            start = b * GROUP * COPM + i * COPM
            out_ref[start : start + COPM, i * CZ : (i + 1) * CZ] = part


def order_kernel(order_ref, mixed_ref, out_ref):
    pick = (order_ref[...] == iota((RES * COPM, RES * COPM), 1)).astype(BF)
    for i in range(2):
        start = BLOCK + i * SIDE
        part = jnp.concatenate([mixed_ref[n, start : start + SIDE, :] for n in range(ROWS)], 0)
        out_ref[:, i * C : (i + 1) * C] = dot(pick, part).astype(BF)


def pair_kernel(quarters, place_ref, res_mask_ref, mask_ref, wide_ref, right_ref, *refs):
    count = len(quarters)
    lefts = refs[:count]
    out_ref, left_ref, mid_ref, done_ref, in_sems, out_sems = refs[-6:]
    gathers = [
        pltpu.make_async_copy(left, left_ref.at[n * QUARTER : (n + 1) * QUARTER, :], in_sems.at[n])
        for n, left in enumerate(lefts)
    ]
    for copy in gathers:
        copy.start()
    row, col = place_ref[0], place_ref[1]
    total = jnp.sum(mask_ref[...].astype(F32), 1, keepdims=True)
    lines = iota((RES, CZ), 0)
    live = jnp.zeros((RES, CZ), F32)
    for j in range(RES):
        live = jnp.where(lines == j, res_mask_ref[col * RES + j].astype(F32), live)
    inverse = 1.0 / jnp.maximum(total * live, 1.0)
    depth, across = col // 8, lax.rem(col // 2, 4)
    residues = []
    for shifted, other in quarters:
        side = lax.rem(col + other, 2)
        place_x = lax.rem(across + 8 - shifted - 2 * lax.rem(row, 2), 4)
        far = lax.rem(place_x + 1, 4) // 2
        for n in range(4):
            source = place_x // 2 * 4 + lax.rem(depth + 4 - n, 4)
            residues.append((2 * far + side) * RES + source * OWN)
    for copy in gathers:
        copy.wait()
    for t in range(count * QUARTER // C):
        block = lax.dot_general(
            right_ref[...], left_ref[t * C : (t + 1) * C, :], (((1,), (1,)), ((), ())), preferred_element_type=F32
        )
        for b in range(COPM):
            rows = block[b * RES : (b + 1) * RES]
            mid_ref[t * 2 * RES : (t + 1) * 2 * RES, b * 128 : (b + 1) * 128] = jnp.concatenate(
                [rows[:, :128], rows[:, 128:]], 0
            ).astype(BF)
    for half in range(2):
        block = dot(mid_ref[...], wide_ref[:, half * C : (half + 1) * C])
        for t in range(len(residues) * OWN // GROUP):
            for i in range(2):
                res = t * GROUP + half * 2 + i
                known = res_mask_ref[row * PAIR_ROWS + residues[res // OWN] + res % OWN]
                scale = jnp.where(known > 0, inverse, 1.0)
                done_ref[res] = block[t * RES : (t + 1) * RES, i * CZ : (i + 1) * CZ] * scale
    copies = [
        pltpu.make_async_copy(
            done_ref.at[n * OWN : (n + 1) * OWN], out_ref.at[pl.ds(residues[n], OWN)], out_sems.at[n]
        )
        for n in range(len(residues))
    ]
    for copy in copies:
        copy.start()
    for copy in copies:
        copy.wait()


def shift(n):
    return [(d, (d + n) % ROWS) for d in range(ROWS)]


def shift_x(n):
    return [(c, c // 8 * 8 + (c + 2 * n) % 8) for c in range(COLS)]


SWAP = [(c, c ^ 1) for c in range(COLS)]


def scatter(depth):
    pairs = []
    for r in range(ROWS):
        for c in range(COLS):
            block, far, core = c // 4, c // 2 % 2, c % 2
            across = (2 * (block % 2) + far + (r // 4 if far else -(r // 4))) % 4
            pairs.append((r * COLS + c, block * COLS + (r + depth) % 4 * 8 + across * 2 + core))
    return pairs


ORDER = np.array(
    [[j // OWN * SIDE + j % OWN * COPM + b] for b in range(COPM) for j in range(RES)], np.int32
)


def shards(
    alignment,
    seq_mask,
    res_mask,
    attn_gain,
    outer_product_gain,
    w_query,
    w_key,
    w_value,
    w_gate,
    output_weight,
    w_left,
    w_right,
    w_pair,
):
    place = jnp.stack([lax.axis_index("row"), lax.axis_index("col")]).astype(jnp.int32)
    tokens = alignment.reshape(SEQ * RES, C)
    mask = seq_mask[None]
    sent = pl.pallas_call(
        norm_kernel,
        out_shape=[jax.ShapeDtypeStruct((BLOCK + 16, C), BF)] * ROWS,
        in_specs=[SMEM, VMEM, VMEM],
        out_specs=[VMEM] * ROWS,
        scratch_shapes=[pltpu.VMEM((SEQ * RES, 128), F32)] * 2,
        compiler_params=pltpu.CompilerParams(vmem_limit_bytes=16 * MIB),
        name="norm",
    )(place, tokens, attn_gain[None])
    blocks = [sent[0]] + [None] * (ROWS - 1)
    for n in FIRST:
        blocks[ROWS - n] = lax.ppermute(sent[n], "row", shift(n))

    wide = pl.pallas_call(
        widen_kernel,
        out_shape=jax.ShapeDtypeStruct((COPM * GROUP * COPM, GROUP * CZ), BF),
        in_specs=[VMEM],
        out_specs=VMEM,
        scratch_shapes=[pltpu.VMEM((COPM * COPM, CZ), F32)],
        compiler_params=pltpu.CompilerParams(vmem_limit_bytes=16 * MIB),
        name="widen",
    )(w_pair)
    mixed, left = pl.pallas_call(
        attend_kernel,
        out_shape=[
            jax.ShapeDtypeStruct((ROWS, BLOCK + 2 * SIDE, C), BF),
            jax.ShapeDtypeStruct((SIDE, TOTAL), BF),
        ],
        in_specs=[SMEM] * 2 + [VMEM] * 18,
        out_specs=[VMEM] * 2,
        scratch_shapes=[pltpu.VMEM((TOTAL, C), BF), pltpu.VMEM((TOTAL, C), F32)],
        compiler_params=pltpu.CompilerParams(vmem_limit_bytes=16 * MIB),
        name="attend",
    )(
        place,
        res_mask,
        *blocks,
        w_query,
        w_key,
        w_value,
        w_gate,
        output_weight,
        attn_gain[None],
        outer_product_gain[None],
        w_left,
        w_right,
        mask,
    )

    mixed = exchanged(mixed)
    along_z = [lax.ppermute(left, ("row", "col"), scatter(n)) for n in range(4)]
    own = {0: jnp.concatenate(along_z, 0)}
    for m in (1, 3, 2):
        own[m] = lax.ppermute(own[0], "col", shift_x(m))
    other = {m: lax.ppermute(own[m], "col", SWAP) for m in range(4)}
    right_all = pl.pallas_call(
        order_kernel,
        out_shape=jax.ShapeDtypeStruct((RES * COPM, TOTAL), BF),
        in_specs=[VMEM] * 2,
        out_specs=VMEM,
        compiler_params=pltpu.CompilerParams(vmem_limit_bytes=16 * MIB),
        name="order",
    )(ORDER, mixed)
    pair = []
    for moves in ((0, 1, 3), (2,)):
        quarters = [(m, side) for m in moves for side in range(2)]
        count = len(quarters)
        pair = [
            pl.pallas_call(
                functools.partial(pair_kernel, quarters),
                out_shape=jax.ShapeDtypeStruct((PAIR_ROWS, RES, CZ), F32),
                in_specs=[SMEM] * 2 + [VMEM] * 3 + [ANY] * (count + len(pair)),
                out_specs=ANY,
                scratch_shapes=[
                    pltpu.VMEM((count * QUARTER, TOTAL), BF),
                    pltpu.VMEM((count * 3 * RES, COPM * GROUP * COPM), BF),
                    pltpu.VMEM((count * 4 * OWN, RES, CZ), F32),
                    pltpu.SemaphoreType.DMA((count,)),
                    pltpu.SemaphoreType.DMA((count * 4,)),
                ],
                input_output_aliases={5 + count: 0} if pair else {},
                compiler_params=pltpu.CompilerParams(vmem_limit_bytes=28 * MIB),
            )(place, res_mask, mask, wide, right_all, *((own, other)[side][m] for m, side in quarters), *pair)
        ]
    added = pl.pallas_call(
        add_kernel,
        out_shape=jax.ShapeDtypeStruct((SEQ * RES, C), F32),
        in_specs=[VMEM] * 3,
        out_specs=VMEM,
        scratch_shapes=[pltpu.VMEM((SEQ * RES, 128), F32)] * 2,
        compiler_params=pltpu.CompilerParams(vmem_limit_bytes=16 * MIB),
        name="add",
    )(tokens, output_weight, mixed)
    return added.reshape(SEQ, RES, C), pair[0]


FIRST = (1, 7, 3, 5, 4, 2, 6)


def exchanged(values):
    return lax.all_to_all(values, "row", split_axis=0, concat_axis=0, tiled=True)


def solution(mesh):
    in_specs = (P("row", "col", None),) + (P(),) * 12
    out_specs = (P("row", "col", None), P("row", "col", None))

    def step(*args):
        return shards(*args)

    step = jax.shard_map(step, mesh=mesh, in_specs=in_specs, out_specs=out_specs, check_vma=False)
    return step
```

```python
import functools

import jax
import jax.numpy as jnp
import numpy as np
from jax import lax
from jax.experimental import pallas as pl
from jax.experimental.pallas import tpu as pltpu
from jax.sharding import PartitionSpec as P


HEAD_DIM = 32
ROWS = 8
COLS = 32
SEQ = 64
RES = 24
OWN = RES // ROWS
TOTAL = SEQ * ROWS
PAIR_ROWS = RES * COLS // ROWS
BLOCK = OWN * SEQ
GROUP = 4
SIDE = OWN * 32
QUARTER = 4 * SIDE
MIB = 1 << 20
C = 256
COPM = 32
CZ = 128
EPS = 1e-05
BF = jnp.bfloat16
F32 = jnp.float32
VMEM = pl.BlockSpec(memory_space=pltpu.VMEM)
SMEM = pl.BlockSpec(memory_space=pltpu.SMEM)
ANY = pl.BlockSpec(memory_space=pl.ANY)


def dot(a, b):
    return jnp.dot(a, b, preferred_element_type=F32)


def iota(shape, dim):
    return lax.broadcasted_iota(jnp.int32, shape, dim)


def column(values):
    return jnp.broadcast_to(values, (8, values.shape[1])).T[:, 0:1]


def norm_kernel(place_ref, align_ref, gain_ref, *refs):
    outs, halves = refs[:ROWS], refs[ROWS:]
    for i in range(2):
        halves[i][...] = align_ref[:, i * 128 : (i + 1) * 128]
    rank = place_ref[0]
    gain = gain_ref[...]
    row = iota((SEQ, 128), 0)
    lane = iota((SEQ, 128), 1)
    row16 = iota((16, 128), 0)
    for n in range(ROWS):
        first = lax.rem(rank + n, ROWS) * OWN
        extra = jnp.zeros((16, 128), F32)
        for j in range(OWN):
            x = jnp.concatenate([half[pl.ds(first + j, SEQ, stride=RES), :] for half in halves], 1)
            centred = x - jnp.mean(x, -1, keepdims=True)
            spread = jnp.mean(centred * centred, -1, keepdims=True) + EPS
            normed = centred * lax.rsqrt(spread) * gain
            outs[n][j * SEQ : (j + 1) * SEQ, :] = normed.astype(BF)
            sigma = jnp.sqrt(spread)
            high = sigma.astype(BF).astype(F32)
            low = sigma - high
            spots = jnp.where(lane == row, high, jnp.where(lane == row + SEQ, low, 0.0))
            extra = extra + jnp.where(row16 == j, jnp.sum(spots, 0, keepdims=True), 0.0)
        outs[n][BLOCK : BLOCK + 16, 0:128] = extra.astype(BF)
        outs[n][BLOCK : BLOCK + 16, 128:256] = jnp.zeros((16, 128), BF)


def attend_kernel(*refs):
    place_ref, res_mask_ref = refs[:2]
    blocks = refs[2:10]
    (wq_ref, wk_ref, wv_ref, wg_ref, wo_ref, gain_ref, gain2_ref, wl_ref, wr_ref, mask_ref) = refs[10:20]
    out_ref, left_ref, gated_ref, gate_ref = refs[20:]
    rank = place_ref[0]
    first_res = place_ref[1] * RES + rank * OWN
    seen = jnp.broadcast_to(mask_ref[...].astype(F32), (8, TOTAL))
    seen = pltpu.roll(seen, lax.rem(ROWS - rank, ROWS) * SEQ, 1)[0:1]
    bias = jnp.where(seen > 0, 0.0, -1000000000.0)
    inv_gain = column(1.0 / gain_ref[...])
    gain2 = column(gain2_ref[...])
    wk, wo = wk_ref[...].T, wo_ref[...].T
    wlr = jnp.concatenate([wl_ref[...].astype(F32), wr_ref[...].astype(F32)], 1).T.astype(BF)
    lane_head = iota((1, C), 1) // HEAD_DIM
    half = iota((1, 128), 1) < SEQ
    tile_head = iota((TOTAL, 128), 1) // HEAD_DIM
    ones = jnp.ones((TOTAL, 128), BF)
    for j in range(OWN):
        x = jnp.concatenate([b[j * SEQ : (j + 1) * SEQ, :] for b in blocks], 0)
        xt = x.T
        queries = (dot(x, wq_ref[...]) * HEAD_DIM**-0.5).astype(BF)
        kt = dot(wk, xt).astype(BF)
        values = dot(x, wv_ref[...]).astype(BF)
        gate_ref[...] = jax.nn.sigmoid(dot(x, wg_ref[...]))
        for tile in range(C // 128):
            lanes = slice(tile * 128, (tile + 1) * 128)
            wide = jnp.concatenate([values[:, lanes], ones], 1)
            mixed = jnp.zeros((TOTAL, 128), F32)
            for h in range(128 // HEAD_DIM):
                picked = (lane_head == tile * (128 // HEAD_DIM) + h).astype(BF)
                logits = dot(queries * picked, kt) + bias
                top = jnp.max(logits, 1, keepdims=True)
                weights = jnp.exp(logits - top).astype(BF)
                both = dot(weights, wide)
                mixed = jnp.where(tile_head == h, both[:, :128] / both[:, 128:], mixed)
            gated_ref[:, lanes] = (mixed * gate_ref[:, lanes]).astype(BF)
        rows = gated_ref[...]
        gated = rows.T
        for p in range(ROWS):
            out_ref[lax.rem(rank + p, ROWS), j * SEQ : (j + 1) * SEQ, :] = rows[p * SEQ : (p + 1) * SEQ, :]
        pieces = []
        for p in range(0, ROWS, 2):
            tiles = []
            for b in blocks[p : p + 2]:
                tile = b[BLOCK : BLOCK + 16, 0:128].astype(F32)[j : j + 1]
                tiles.append(tile + pltpu.roll(tile, SEQ, 1))
            pieces.append(jnp.where(half, tiles[0], tiles[1]))
        sigma = jnp.concatenate(pieces, 1)
        y = dot(wo, gated) + xt.astype(F32) * inv_gain * sigma
        centred = y - jnp.mean(y, 0, keepdims=True)
        spread = jnp.mean(centred * centred, 0, keepdims=True)
        second = (centred * lax.rsqrt(spread + EPS) * gain2).astype(BF)
        live = res_mask_ref[first_res + j].astype(F32)
        sides = dot(wlr, second) * (seen * live)
        sides = pltpu.roll(sides, rank * SEQ, 1).astype(BF)
        left_ref[j * COPM : (j + 1) * COPM, :] = sides[:COPM]
        for p in range(ROWS):
            for i in range(2):
                spot = BLOCK + i * SIDE + j * COPM
                out_ref[p, spot : spot + COPM, :] = sides[COPM:, i * C : (i + 1) * C]


def add_kernel(align_ref, wo_ref, mixed_ref, out_ref, *halves):
    for n in range(ROWS):
        delta = dot(mixed_ref[n, 0:BLOCK, :], wo_ref[...])
        for j in range(OWN):
            for i in range(2):
                part = delta[j * SEQ : (j + 1) * SEQ, i * 128 : (i + 1) * 128]
                halves[i][pl.ds(n * OWN + j, SEQ, stride=RES), :] = part
    for i in range(2):
        lanes = slice(i * 128, (i + 1) * 128)
        out_ref[:, lanes] = align_ref[:, lanes] + halves[i][...]


def widen_kernel(w_ref, out_ref, wide_ref):
    wide_ref[...] = w_ref[...].astype(F32)
    out_ref[...] = jnp.zeros(out_ref.shape, BF)
    for b in range(COPM):
        part = wide_ref[pl.ds(b, COPM, stride=COPM), :].astype(BF)
        for i in range(GROUP):
            start = b * GROUP * COPM + i * COPM
            out_ref[start : start + COPM, i * CZ : (i + 1) * CZ] = part


def order_kernel(order_ref, mixed_ref, out_ref):
    pick = (order_ref[...] == iota((RES * COPM, RES * COPM), 1)).astype(BF)
    for i in range(2):
        start = BLOCK + i * SIDE
        part = jnp.concatenate([mixed_ref[n, start : start + SIDE, :] for n in range(ROWS)], 0)
        out_ref[:, i * C : (i + 1) * C] = dot(pick, part).astype(BF)


def pair_kernel(quarters, place_ref, res_mask_ref, mask_ref, wide_ref, right_ref, *refs):
    count = len(quarters)
    lefts = refs[:count]
    out_ref, left_ref, mid_ref, done_ref, in_sems, out_sems = refs[-6:]
    gathers = [
        pltpu.make_async_copy(left, left_ref.at[n * QUARTER : (n + 1) * QUARTER, :], in_sems.at[n])
        for n, left in enumerate(lefts)
    ]
    for copy in gathers:
        copy.start()
    row, col = place_ref[0], place_ref[1]
    total = jnp.sum(mask_ref[...].astype(F32), 1, keepdims=True)
    lines = iota((RES, CZ), 0)
    live = jnp.zeros((RES, CZ), F32)
    for j in range(RES):
        live = jnp.where(lines == j, res_mask_ref[col * RES + j].astype(F32), live)
    inverse = 1.0 / jnp.maximum(total * live, 1.0)
    depth, across = col // 8, lax.rem(col // 2, 4)
    residues = []
    for shifted, other in quarters:
        side = lax.rem(col + other, 2)
        place_x = lax.rem(across + 8 - shifted - 2 * lax.rem(row, 2), 4)
        far = lax.rem(place_x + 1, 4) // 2
        for n in range(4):
            source = place_x // 2 * 4 + lax.rem(depth + 4 - n, 4)
            residues.append((2 * far + side) * RES + source * OWN)
    landed = 0
    copies = []
    tiles = count * QUARTER // C
    for part in range(2):
        for t in range(part * tiles // 2, (part + 1) * tiles // 2):
            while landed * QUARTER < (t + 1) * C:
                gathers[landed].wait()
                landed += 1
            block = lax.dot_general(
                right_ref[...],
                left_ref[t * C : (t + 1) * C, :],
                (((1,), (1,)), ((), ())),
                preferred_element_type=F32,
            )
            for b in range(COPM):
                rows = block[b * RES : (b + 1) * RES]
                mid_ref[t * 2 * RES : (t + 1) * 2 * RES, b * 128 : (b + 1) * 128] = jnp.concatenate(
                    [rows[:, :128], rows[:, 128:]], 0
                ).astype(BF)
        groups = range(part * tiles, (part + 1) * tiles)
        for half in range(2):
            block = dot(mid_ref[groups[0] * RES : (groups[-1] + 1) * RES, :], wide_ref[:, half * C : (half + 1) * C])
            for k, t in enumerate(groups):
                for i in range(2):
                    res = t * GROUP + half * 2 + i
                    known = res_mask_ref[row * PAIR_ROWS + residues[res // OWN] + res % OWN]
                    scale = jnp.where(known > 0, inverse, 1.0)
                    done_ref[res] = block[k * RES : (k + 1) * RES, i * CZ : (i + 1) * CZ] * scale
        for n in range(groups[0] * GROUP // OWN, (groups[-1] + 1) * GROUP // OWN):
            copies.append(
                pltpu.make_async_copy(
                    done_ref.at[n * OWN : (n + 1) * OWN], out_ref.at[pl.ds(residues[n], OWN)], out_sems.at[n]
                )
            )
            copies[-1].start()
    for copy in copies:
        copy.wait()


def shift(n):
    return [(d, (d + n) % ROWS) for d in range(ROWS)]


def shift_x(n):
    return [(c, c // 8 * 8 + (c + 2 * n) % 8) for c in range(COLS)]


SWAP = [(c, c ^ 1) for c in range(COLS)]


def scatter(depth):
    pairs = []
    for r in range(ROWS):
        for c in range(COLS):
            block, far, core = c // 4, c // 2 % 2, c % 2
            across = (2 * (block % 2) + far + (r // 4 if far else -(r // 4))) % 4
            pairs.append((r * COLS + c, block * COLS + (r + depth) % 4 * 8 + across * 2 + core))
    return pairs


ORDER = np.array(
    [[j // OWN * SIDE + j % OWN * COPM + b] for b in range(COPM) for j in range(RES)], np.int32
)


def shards(
    alignment,
    seq_mask,
    res_mask,
    attn_gain,
    outer_product_gain,
    w_query,
    w_key,
    w_value,
    w_gate,
    output_weight,
    w_left,
    w_right,
    w_pair,
):
    place = jnp.stack([lax.axis_index("row"), lax.axis_index("col")]).astype(jnp.int32)
    tokens = alignment.reshape(SEQ * RES, C)
    mask = seq_mask[None]
    sent = pl.pallas_call(
        norm_kernel,
        out_shape=[jax.ShapeDtypeStruct((BLOCK + 16, C), BF)] * ROWS,
        in_specs=[SMEM, VMEM, VMEM],
        out_specs=[VMEM] * ROWS,
        scratch_shapes=[pltpu.VMEM((SEQ * RES, 128), F32)] * 2,
        compiler_params=pltpu.CompilerParams(vmem_limit_bytes=16 * MIB),
        name="norm",
    )(place, tokens, attn_gain[None])
    blocks = [sent[0]] + [None] * (ROWS - 1)
    for n in FIRST:
        blocks[ROWS - n] = lax.ppermute(sent[n], "row", shift(n))

    wide = pl.pallas_call(
        widen_kernel,
        out_shape=jax.ShapeDtypeStruct((COPM * GROUP * COPM, GROUP * CZ), BF),
        in_specs=[VMEM],
        out_specs=VMEM,
        scratch_shapes=[pltpu.VMEM((COPM * COPM, CZ), F32)],
        compiler_params=pltpu.CompilerParams(vmem_limit_bytes=16 * MIB),
        name="widen",
    )(w_pair)
    mixed, left = pl.pallas_call(
        attend_kernel,
        out_shape=[
            jax.ShapeDtypeStruct((ROWS, BLOCK + 2 * SIDE, C), BF),
            jax.ShapeDtypeStruct((SIDE, TOTAL), BF),
        ],
        in_specs=[SMEM] * 2 + [VMEM] * 18,
        out_specs=[VMEM] * 2,
        scratch_shapes=[pltpu.VMEM((TOTAL, C), BF), pltpu.VMEM((TOTAL, C), F32)],
        compiler_params=pltpu.CompilerParams(vmem_limit_bytes=16 * MIB),
        name="attend",
    )(
        place,
        res_mask,
        *blocks,
        w_query,
        w_key,
        w_value,
        w_gate,
        output_weight,
        attn_gain[None],
        outer_product_gain[None],
        w_left,
        w_right,
        mask,
    )

    mixed = exchanged(mixed)
    along_z = [lax.ppermute(left, ("row", "col"), scatter(n)) for n in range(4)]
    own = {0: jnp.concatenate(along_z, 0)}
    for m in (1, 3, 2):
        own[m] = lax.ppermute(own[0], "col", shift_x(m))
    other = {m: lax.ppermute(own[m], "col", SWAP) for m in range(4)}
    right_all = pl.pallas_call(
        order_kernel,
        out_shape=jax.ShapeDtypeStruct((RES * COPM, TOTAL), BF),
        in_specs=[VMEM] * 2,
        out_specs=VMEM,
        compiler_params=pltpu.CompilerParams(vmem_limit_bytes=16 * MIB),
        name="order",
    )(ORDER, mixed)
    quarters = [(m, side) for m in (0, 1, 3, 2) for side in range(2)]
    count = len(quarters)
    pair = pl.pallas_call(
        functools.partial(pair_kernel, quarters),
        out_shape=jax.ShapeDtypeStruct((PAIR_ROWS, RES, CZ), F32),
        in_specs=[SMEM] * 2 + [VMEM] * 3 + [ANY] * count,
        out_specs=ANY,
        scratch_shapes=[
            pltpu.VMEM((count * QUARTER, TOTAL), BF),
            pltpu.VMEM((count * 3 * RES, COPM * GROUP * COPM), BF),
            pltpu.VMEM((count * 4 * OWN, RES, CZ), F32),
            pltpu.SemaphoreType.DMA((count,)),
            pltpu.SemaphoreType.DMA((count * 4,)),
        ],
        compiler_params=pltpu.CompilerParams(vmem_limit_bytes=28 * MIB),
        name="pair",
    )(place, res_mask, mask, wide, right_all, *((own, other)[side][m] for m, side in quarters))
    added = pl.pallas_call(
        add_kernel,
        out_shape=jax.ShapeDtypeStruct((SEQ * RES, C), F32),
        in_specs=[VMEM] * 3,
        out_specs=VMEM,
        scratch_shapes=[pltpu.VMEM((SEQ * RES, 128), F32)] * 2,
        compiler_params=pltpu.CompilerParams(vmem_limit_bytes=16 * MIB),
        name="add",
    )(tokens, output_weight, mixed)
    return added.reshape(SEQ, RES, C), pair


FIRST = (1, 7, 3, 5, 4, 2, 6)


def exchanged(values):
    return lax.all_to_all(values, "row", split_axis=0, concat_axis=0, tiled=True)


def solution(mesh):
    in_specs = (P("row", "col", None),) + (P(),) * 12
    out_specs = (P("row", "col", None), P("row", "col", None))

    def step(*args):
        return shards(*args)

    step = jax.shard_map(step, mesh=mesh, in_specs=in_specs, out_specs=out_specs, check_vma=False)
    return step
```

```python
import functools

import jax
import jax.numpy as jnp
from jax import lax
from jax.experimental import pallas as pl
from jax.experimental.pallas import tpu as pltpu
from jax.sharding import PartitionSpec as P


HEAD_DIM = 32
ROWS = 8
COLS = 32
SEQ = 64
RES = 24
OWN = RES // ROWS
TOTAL = SEQ * ROWS
PAIR_ROWS = RES * COLS // ROWS
BLOCK = OWN * SEQ
GROUP = 4
SIDE = OWN * 32
QUARTER = 4 * SIDE
MIB = 1 << 20
C = 256
COPM = 32
CZ = 128
EPS = 1e-05
BF = jnp.bfloat16
F32 = jnp.float32
VMEM = pl.BlockSpec(memory_space=pltpu.VMEM)
SMEM = pl.BlockSpec(memory_space=pltpu.SMEM)
ANY = pl.BlockSpec(memory_space=pl.ANY)


def dot(a, b):
    return jnp.dot(a, b, preferred_element_type=F32)


def iota(shape, dim):
    return lax.broadcasted_iota(jnp.int32, shape, dim)


def column(values):
    return jnp.broadcast_to(values, (8, values.shape[1])).T[:, 0:1]


def norm_kernel(place_ref, align_ref, gain_ref, *refs):
    outs, halves = refs[:ROWS], refs[ROWS:]
    for i in range(2):
        halves[i][...] = align_ref[:, i * 128 : (i + 1) * 128]
    rank = place_ref[0]
    gain = gain_ref[...]
    row = iota((SEQ, 128), 0)
    lane = iota((SEQ, 128), 1)
    row16 = iota((16, 128), 0)
    for n in range(ROWS):
        first = lax.rem(rank + n, ROWS) * OWN
        extra = jnp.zeros((16, 128), F32)
        for j in range(OWN):
            x = jnp.concatenate([half[pl.ds(first + j, SEQ, stride=RES), :] for half in halves], 1)
            centred = x - jnp.mean(x, -1, keepdims=True)
            spread = jnp.mean(centred * centred, -1, keepdims=True) + EPS
            normed = centred * lax.rsqrt(spread) * gain
            outs[n][j * SEQ : (j + 1) * SEQ, :] = normed.astype(BF)
            sigma = jnp.sqrt(spread)
            high = sigma.astype(BF).astype(F32)
            low = sigma - high
            spots = jnp.where(lane == row, high, jnp.where(lane == row + SEQ, low, 0.0))
            extra = extra + jnp.where(row16 == j, jnp.sum(spots, 0, keepdims=True), 0.0)
        outs[n][BLOCK : BLOCK + 16, 0:128] = extra.astype(BF)
        outs[n][BLOCK : BLOCK + 16, 128:256] = jnp.zeros((16, 128), BF)


def attend_kernel(*refs):
    place_ref, res_mask_ref = refs[:2]
    blocks = refs[2:10]
    (wq_ref, wk_ref, wv_ref, wg_ref, wo_ref, gain_ref, gain2_ref, wl_ref, wr_ref, mask_ref) = refs[10:20]
    out_ref, left_ref, gated_ref, gate_ref = refs[20:]
    rank = place_ref[0]
    first_res = place_ref[1] * RES + rank * OWN
    seen = jnp.broadcast_to(mask_ref[...].astype(F32), (8, TOTAL))
    seen = pltpu.roll(seen, lax.rem(ROWS - rank, ROWS) * SEQ, 1)[0:1]
    bias = jnp.where(seen > 0, 0.0, -1000000000.0)
    inv_gain = column(1.0 / gain_ref[...])
    gain2 = column(gain2_ref[...])
    wk, wo = wk_ref[...].T, wo_ref[...].T
    wlr = jnp.concatenate([wl_ref[...].astype(F32), wr_ref[...].astype(F32)], 1).T.astype(BF)
    lane_head = iota((1, C), 1) // HEAD_DIM
    half = iota((1, 128), 1) < SEQ
    tile_head = iota((TOTAL, 128), 1) // HEAD_DIM
    ones = jnp.ones((TOTAL, 128), BF)
    for j in range(OWN):
        x = jnp.concatenate([b[j * SEQ : (j + 1) * SEQ, :] for b in blocks], 0)
        xt = x.T
        queries = (dot(x, wq_ref[...]) * HEAD_DIM**-0.5).astype(BF)
        kt = dot(wk, xt).astype(BF)
        values = dot(x, wv_ref[...]).astype(BF)
        gate_ref[...] = jax.nn.sigmoid(dot(x, wg_ref[...]))
        for tile in range(C // 128):
            lanes = slice(tile * 128, (tile + 1) * 128)
            wide = jnp.concatenate([values[:, lanes], ones], 1)
            mixed = jnp.zeros((TOTAL, 128), F32)
            for h in range(128 // HEAD_DIM):
                picked = (lane_head == tile * (128 // HEAD_DIM) + h).astype(BF)
                logits = dot(queries * picked, kt) + bias
                top = jnp.max(logits, 1, keepdims=True)
                weights = jnp.exp(logits - top).astype(BF)
                both = dot(weights, wide)
                mixed = jnp.where(tile_head == h, both[:, :128] / both[:, 128:], mixed)
            gated_ref[:, lanes] = (mixed * gate_ref[:, lanes]).astype(BF)
        rows = gated_ref[...]
        gated = rows.T
        for p in range(ROWS):
            out_ref[lax.rem(rank + p, ROWS), j * SEQ : (j + 1) * SEQ, :] = rows[p * SEQ : (p + 1) * SEQ, :]
        pieces = []
        for p in range(0, ROWS, 2):
            tiles = []
            for b in blocks[p : p + 2]:
                tile = b[BLOCK : BLOCK + 16, 0:128].astype(F32)[j : j + 1]
                tiles.append(tile + pltpu.roll(tile, SEQ, 1))
            pieces.append(jnp.where(half, tiles[0], tiles[1]))
        sigma = jnp.concatenate(pieces, 1)
        y = dot(wo, gated) + xt.astype(F32) * inv_gain * sigma
        centred = y - jnp.mean(y, 0, keepdims=True)
        spread = jnp.mean(centred * centred, 0, keepdims=True)
        second = (centred * lax.rsqrt(spread + EPS) * gain2).astype(BF)
        live = res_mask_ref[first_res + j].astype(F32)
        sides = dot(wlr, second) * (seen * live)
        sides = pltpu.roll(sides, rank * SEQ, 1).astype(BF)
        left_ref[j * COPM : (j + 1) * COPM, :] = sides[:COPM]
        for p in range(ROWS):
            for i in range(2):
                spot = BLOCK + i * SIDE + j * COPM
                out_ref[p, spot : spot + COPM, :] = sides[COPM:, i * C : (i + 1) * C]


def add_kernel(align_ref, wo_ref, mixed_ref, out_ref, *halves):
    for n in range(ROWS):
        delta = dot(mixed_ref[n, 0:BLOCK, :], wo_ref[...])
        for j in range(OWN):
            for i in range(2):
                part = delta[j * SEQ : (j + 1) * SEQ, i * 128 : (i + 1) * 128]
                halves[i][pl.ds(n * OWN + j, SEQ, stride=RES), :] = part
    for i in range(2):
        lanes = slice(i * 128, (i + 1) * 128)
        out_ref[:, lanes] = align_ref[:, lanes] + halves[i][...]


def widen_kernel(w_ref, out_ref, wide_ref):
    wide_ref[...] = w_ref[...].astype(F32)
    out_ref[...] = jnp.zeros(out_ref.shape, BF)
    for b in range(COPM):
        part = wide_ref[pl.ds(b, COPM, stride=COPM), :].astype(BF)
        for i in range(GROUP):
            start = b * GROUP * COPM + i * COPM
            out_ref[start : start + COPM, i * CZ : (i + 1) * CZ] = part


def order_kernel(mixed_ref, out_ref):
    place = iota((RES * COPM, 128), 0)[:, 0:1].astype(F32)
    channel = jnp.floor((place + 0.5) * (1.0 / RES))
    residue = place - channel * RES
    device = jnp.floor((residue + 0.5) * (1.0 / OWN))
    source = (device * SIDE + (residue - device * OWN) * COPM + channel).astype(jnp.int32)
    pick = (source == iota((RES * COPM, RES * COPM), 1)).astype(BF)
    for i in range(2):
        start = BLOCK + i * SIDE
        part = jnp.concatenate([mixed_ref[n, start : start + SIDE, :] for n in range(ROWS)], 0)
        out_ref[:, i * C : (i + 1) * C] = dot(pick, part).astype(BF)


def pair_kernel(quarters, place_ref, res_mask_ref, mask_ref, wide_ref, right_ref, *refs):
    count = len(quarters)
    lefts = refs[:count]
    out_ref, left_ref, mid_ref, done_ref, in_sems, out_sems = refs[-6:]
    gathers = [
        pltpu.make_async_copy(left, left_ref.at[n * QUARTER : (n + 1) * QUARTER, :], in_sems.at[n])
        for n, left in enumerate(lefts)
    ]
    for copy in gathers:
        copy.start()
    row, col = place_ref[0], place_ref[1]
    total = jnp.sum(mask_ref[...].astype(F32), 1, keepdims=True)
    lines = iota((RES, CZ), 0)
    live = jnp.zeros((RES, CZ), F32)
    for j in range(RES):
        live = jnp.where(lines == j, res_mask_ref[col * RES + j].astype(F32), live)
    inverse = 1.0 / jnp.maximum(total * live, 1.0)
    depth, across = col // 8, lax.rem(col // 2, 4)
    residues = []
    for shifted, other in quarters:
        side = lax.rem(col + other, 2)
        place_x = lax.rem(across + 8 - shifted - 2 * lax.rem(row, 2), 4)
        far = lax.rem(place_x + 1, 4) // 2
        for n in range(4):
            source = place_x // 2 * 4 + lax.rem(depth + 4 - n, 4)
            residues.append((2 * far + side) * RES + source * OWN)
    landed = 0
    copies = []
    tiles = count * QUARTER // C
    for part in range(2):
        for t in range(part * tiles // 2, (part + 1) * tiles // 2):
            while landed * QUARTER < (t + 1) * C:
                gathers[landed].wait()
                landed += 1
            block = lax.dot_general(
                right_ref[...],
                left_ref[t * C : (t + 1) * C, :],
                (((1,), (1,)), ((), ())),
                preferred_element_type=F32,
            )
            for b in range(COPM):
                rows = block[b * RES : (b + 1) * RES]
                mid_ref[t * 2 * RES : (t + 1) * 2 * RES, b * 128 : (b + 1) * 128] = jnp.concatenate(
                    [rows[:, :128], rows[:, 128:]], 0
                ).astype(BF)
        groups = range(part * tiles, (part + 1) * tiles)
        for half in range(2):
            block = dot(mid_ref[groups[0] * RES : (groups[-1] + 1) * RES, :], wide_ref[:, half * C : (half + 1) * C])
            for k, t in enumerate(groups):
                for i in range(2):
                    res = t * GROUP + half * 2 + i
                    known = res_mask_ref[row * PAIR_ROWS + residues[res // OWN] + res % OWN]
                    scale = jnp.where(known > 0, inverse, 1.0)
                    done_ref[res] = block[k * RES : (k + 1) * RES, i * CZ : (i + 1) * CZ] * scale
        for n in range(groups[0] * GROUP // OWN, (groups[-1] + 1) * GROUP // OWN):
            copies.append(
                pltpu.make_async_copy(
                    done_ref.at[n * OWN : (n + 1) * OWN], out_ref.at[pl.ds(residues[n], OWN)], out_sems.at[n]
                )
            )
            copies[-1].start()
    for copy in copies:
        copy.wait()


def shift(n):
    return [(d, (d + n) % ROWS) for d in range(ROWS)]


def shift_x(n):
    return [(c, c // 8 * 8 + (c + 2 * n) % 8) for c in range(COLS)]


SWAP = [(c, c ^ 1) for c in range(COLS)]


def scatter(depth):
    pairs = []
    for r in range(ROWS):
        for c in range(COLS):
            block, far, core = c // 4, c // 2 % 2, c % 2
            across = (2 * (block % 2) + far + (r // 4 if far else -(r // 4))) % 4
            pairs.append((r * COLS + c, block * COLS + (r + depth) % 4 * 8 + across * 2 + core))
    return pairs


def shards(
    alignment,
    seq_mask,
    res_mask,
    attn_gain,
    outer_product_gain,
    w_query,
    w_key,
    w_value,
    w_gate,
    output_weight,
    w_left,
    w_right,
    w_pair,
):
    place = jnp.stack([lax.axis_index("row"), lax.axis_index("col")]).astype(jnp.int32)
    tokens = alignment.reshape(SEQ * RES, C)
    mask = seq_mask[None]
    sent = pl.pallas_call(
        norm_kernel,
        out_shape=[jax.ShapeDtypeStruct((BLOCK + 16, C), BF)] * ROWS,
        in_specs=[SMEM, VMEM, VMEM],
        out_specs=[VMEM] * ROWS,
        scratch_shapes=[pltpu.VMEM((SEQ * RES, 128), F32)] * 2,
        compiler_params=pltpu.CompilerParams(vmem_limit_bytes=16 * MIB),
        name="norm",
    )(place, tokens, attn_gain[None])
    blocks = [sent[0]] + [None] * (ROWS - 1)
    for n in FIRST:
        blocks[ROWS - n] = lax.ppermute(sent[n], "row", shift(n))

    wide = pl.pallas_call(
        widen_kernel,
        out_shape=jax.ShapeDtypeStruct((COPM * GROUP * COPM, GROUP * CZ), BF),
        in_specs=[VMEM],
        out_specs=VMEM,
        scratch_shapes=[pltpu.VMEM((COPM * COPM, CZ), F32)],
        compiler_params=pltpu.CompilerParams(vmem_limit_bytes=16 * MIB),
        name="widen",
    )(w_pair)
    mixed, left = pl.pallas_call(
        attend_kernel,
        out_shape=[
            jax.ShapeDtypeStruct((ROWS, BLOCK + 2 * SIDE, C), BF),
            jax.ShapeDtypeStruct((SIDE, TOTAL), BF),
        ],
        in_specs=[SMEM] * 2 + [VMEM] * 18,
        out_specs=[VMEM] * 2,
        scratch_shapes=[pltpu.VMEM((TOTAL, C), BF), pltpu.VMEM((TOTAL, C), F32)],
        compiler_params=pltpu.CompilerParams(vmem_limit_bytes=16 * MIB),
        name="attend",
    )(
        place,
        res_mask,
        *blocks,
        w_query,
        w_key,
        w_value,
        w_gate,
        output_weight,
        attn_gain[None],
        outer_product_gain[None],
        w_left,
        w_right,
        mask,
    )

    mixed = exchanged(mixed)
    along_z = [lax.ppermute(left, ("row", "col"), scatter(n)) for n in range(4)]
    own = {0: jnp.concatenate(along_z, 0)}
    for m in (1, 3, 2):
        own[m] = lax.ppermute(own[0], "col", shift_x(m))
    other = {m: lax.ppermute(own[m], "col", SWAP) for m in range(4)}
    right_all = pl.pallas_call(
        order_kernel,
        out_shape=jax.ShapeDtypeStruct((RES * COPM, TOTAL), BF),
        in_specs=[VMEM],
        out_specs=VMEM,
        compiler_params=pltpu.CompilerParams(vmem_limit_bytes=16 * MIB),
        name="order",
    )(mixed)
    quarters = [(m, side) for m in (0, 1, 3, 2) for side in range(2)]
    count = len(quarters)
    pair = pl.pallas_call(
        functools.partial(pair_kernel, quarters),
        out_shape=jax.ShapeDtypeStruct((PAIR_ROWS, RES, CZ), F32),
        in_specs=[SMEM] * 2 + [VMEM] * 3 + [ANY] * count,
        out_specs=ANY,
        scratch_shapes=[
            pltpu.VMEM((count * QUARTER, TOTAL), BF),
            pltpu.VMEM((count * 3 * RES, COPM * GROUP * COPM), BF),
            pltpu.VMEM((count * 4 * OWN, RES, CZ), F32),
            pltpu.SemaphoreType.DMA((count,)),
            pltpu.SemaphoreType.DMA((count * 4,)),
        ],
        compiler_params=pltpu.CompilerParams(vmem_limit_bytes=28 * MIB),
        name="pair",
    )(place, res_mask, mask, wide, right_all, *((own, other)[side][m] for m, side in quarters))
    added = pl.pallas_call(
        add_kernel,
        out_shape=jax.ShapeDtypeStruct((SEQ * RES, C), F32),
        in_specs=[VMEM] * 3,
        out_specs=VMEM,
        scratch_shapes=[pltpu.VMEM((SEQ * RES, 128), F32)] * 2,
        compiler_params=pltpu.CompilerParams(vmem_limit_bytes=16 * MIB),
        name="add",
    )(tokens, output_weight, mixed)
    return added.reshape(SEQ, RES, C), pair


FIRST = (1, 7, 3, 5, 4, 2, 6)


def exchanged(values):
    return lax.all_to_all(values, "row", split_axis=0, concat_axis=0, tiled=True)


def solution(mesh):
    in_specs = (P("row", "col", None),) + (P(),) * 12
    out_specs = (P("row", "col", None), P("row", "col", None))

    def step(*args):
        return shards(*args)

    step = jax.shard_map(step, mesh=mesh, in_specs=in_specs, out_specs=out_specs, check_vma=False)
    return step
```
